128 devices in a mesh: gx: 16 (over x_lo, y, core), gy: 8 (over z, x_hi).
Axes of the slice: x: 4 (x_hi: 2, x_lo: 2; x = x_hi * 2 + x_lo), y: 4, z: 4, core: 2. Of those that a mesh axis runs over, the one named last changes fastest.
Arguments:
- collocation: bfloat16 [3072, 16384], P(None, 'gx'), may hold values from -6 to 6
- density: bfloat16 [3072, 3072], P('gy'), may hold values from -0.109375 to 0.109375
- kernel: bfloat16 [16384, 16, 8, 128], P('gx', None, 'gy'), may hold values from -6.67572e-06 to 6.67572e-06
Outputs:
- exchange: float32 [3072, 3072], P('gx', 'gy')
The draws below stay inside these ranges and needn't reach their ends.
All inputs are finite; a program needn't handle non-finite values.
Results may differ from the reference program's by a relative error of at most 0.008.
Values may be sent and summed in bfloat16 or wider, within the bound.
A program may use at most 448 MiB of HBM per device.

```python
import jax
import jax.numpy as jnp
from jax import lax

NBF = 3072
NPTS = 16384
CYCLE_LEN = 16
COL_GROUPS = 8
PIECE = 128
N_GX = 16


def block_levels(stream_key, shape, pieces, smallest, high):
    factor_of, own = 1.0, jax.random.fold_in(stream_key, 6)
    for dim, blocks in pieces:
        steps = jnp.exp(jax.random.uniform(jax.random.fold_in(own, dim), (blocks,), jnp.float32, smallest / len(pieces), high / len(pieces)))
        factor_of = factor_of * jnp.repeat(steps, shape[dim] // blocks).reshape([-1 if axis == dim else 1 for axis in range(len(shape))])
    return factor_of


def noise(rng, shape, deviation, limit, cuts=(), held_as=jnp.bfloat16):
    values = deviation * jax.random.normal(rng, shape, jnp.float32)
    if cuts:
        values = values * block_levels(rng, shape, cuts, -0.22, 0.18)
    return jnp.clip(values, -limit, limit).astype(held_as)


def setup_inputs(seed: int = 0) -> dict:
    key_list = jax.random.split(jax.random.key(seed), 4)
    collocation = noise(key_list[0], (NBF, NPTS), 1.0, 6.0, ((1, 16),))
    density = noise(key_list[1], (NBF, NBF), NBF ** -0.5, 0.109375, ((0, 8),))
    kernel = noise(key_list[2], (NPTS, CYCLE_LEN, COL_GROUPS, PIECE), (NPTS * NPTS * NBF) ** -0.5, 6.67572021484375e-06, ((0, 16), (2, 8)))
    return {"collocation": collocation, "density": density, "kernel": kernel}


def reference(collocation, density, kernel):
    dense = jnp.dot(density, collocation, preferred_element_type=jnp.float32).astype(jnp.bfloat16)
    flat_kernel = kernel.reshape(NPTS, NPTS)
    block_len = NPTS // N_GX

    def scan_step(running, position):
        offset = (position * block_len).astype(jnp.int32)
        dense_rows = lax.dynamic_slice_in_dim(dense, offset, block_len, 1)
        colloc_rows = lax.dynamic_slice_in_dim(collocation, offset, block_len, 1)
        coefficients = lax.dynamic_slice_in_dim(flat_kernel, offset, block_len, 0)
        products = jnp.dot(dense_rows.T, collocation, preferred_element_type=jnp.float32)
        weighted = (coefficients.astype(jnp.float32) * products).astype(jnp.bfloat16)
        contracted = jnp.dot(weighted, collocation.T, preferred_element_type=jnp.float32).astype(jnp.bfloat16)
        return running + jnp.dot(colloc_rows, contracted, preferred_element_type=jnp.float32), None

    running, unused = lax.scan(scan_step, jnp.zeros((NBF, NBF), jnp.float32), jnp.arange(N_GX, dtype=jnp.int32))
    return running
```

```python
import jax
import jax.numpy as jnp
from jax import lax
from jax.experimental import pallas as pl
from jax.experimental.pallas import tpu as pltpu
from jax.sharding import PartitionSpec as P

MESH = pl.DeviceIdType.MESH
BF16 = jnp.bfloat16
F32 = jnp.float32

NBF = 3072
PANEL = 1024
PIECE = 128
ROWS = 384
NQ = 2048
HALF = NBF // 2
CORE_ROWS = 192
N_SENDS = 120


def dot(a, b):
    return jnp.dot(a, b, preferred_element_type=F32)


def kernel(
    c_ref, d_ref, z_ref, out_ref,
    cp, dv, dt, cq, zw, rel, dr, rin1, rf1, rin2, rf2, rin3, rf3,
    send_sem, recv_sem, local_sem,
):
    gx, gy = lax.axis_index("gx"), lax.axis_index("gy")
    c, y, xl = gx % 2, (gx // 2) % 4, gx // 8
    z, xh = gy // 2, gy % 2
    x = xh * 2 + xl

    def device(x, y, z, c):
        return {"gx": ((x % 2) * 4 + y) * 2 + c, "gy": z * 2 + x // 2}

    def up(v):
        return (v + 1) % 4

    def down(v):
        return (v + 3) % 4

    partner = device(x, y, z, 1 - c)
    x_up, x_dn = device(up(x), y, z, c), device(down(x), y, z, c)
    y_up, y_dn = device(x, up(y), z, c), device(x, down(y), z, c)
    z_up, z_dn = device(x, y, up(z), c), device(x, y, down(z), c)

    barrier = pltpu.get_barrier_semaphore()
    neighbours = (partner, x_up, x_dn, y_up, y_dn, z_up, z_dn)
    for one in neighbours:
        pl.semaphore_signal(barrier, inc=1, device_id=one, device_id_type=MESH)

    locals_ = []

    def fetch(src, dst):
        copy = pltpu.make_async_copy(src, dst, local_sem.at[len(locals_)])
        copy.start()
        locals_.append(copy)
        return copy

    def column(ref, k, rows=None, width=PIECE):
        cols = pl.ds(pl.multiple_of(k * width, PIECE), width)
        return ref.at[:, cols] if rows is None else ref.at[pl.ds(*rows), cols]

    d_in = fetch(d_ref, dv)
    cp_in = [fetch(column(c_ref, i, width=256), column(cp, i, width=256)) for i in range(4)]
    own_in = fetch(column(c_ref, gy), column(cq, gx))
    z_in = fetch(z_ref, zw)
    pl.semaphore_wait(barrier, len(neighbours))

    sent = []

    def send(src, dst, to, lands):
        i = len(sent)
        copy = pltpu.make_async_remote_copy(
            src_ref=src, dst_ref=dst, send_sem=send_sem.at[i], recv_sem=recv_sem.at[i],
            device_id=to, device_id_type=MESH,
        )
        copy.start()
        sent.append(copy)
        arrival = pltpu.make_async_remote_copy(
            src_ref=lands, dst_ref=lands, send_sem=send_sem.at[i], recv_sem=recv_sem.at[i],
            device_id=to, device_id_type=MESH,
        )
        return arrival.wait_recv

    def slot(xl, y, c):
        return (xl * 4 + y) * 2 + c

    low, high = (0, HALF), (HALF, HALF)

    def piece(k, rows=None):
        return column(cq, k, rows)

    def relay_piece(k, to, mine, rows=None):
        return send(piece(k, rows), piece(k, rows), to, piece(mine, rows))

    own = column(c_ref, gy)
    y_own_dn = send(own, piece(gx), y_up, piece(slot(xl, down(y), c)))
    y_own_up = send(own, piece(gx), y_dn, piece(slot(xl, up(y), c)))
    other = slot(1 - xl, y, c)
    x_lo = send(column(c_ref, z * 2 + up(x) // 2, low), piece(gx, low), x_up, piece(other, low))
    x_hi = send(column(c_ref, z * 2 + down(x) // 2, high), piece(gx, high), x_dn, piece(other, high))
    done = [send(own, piece(gx), partner, piece(slot(xl, y, 1 - c)))]

    def block(j, h):
        return dt.at[pl.ds(h * 512, 512), pl.ds(pl.multiple_of(j * ROWS, PIECE), ROWS)]

    def group(x, z):
        return z * 2 + x // 2

    own_cols = pl.ds(pl.multiple_of(gy * ROWS, PIECE), ROWS)
    d_in.wait()
    z_own_dn, z_own_up, relayed = [], [], []
    for i in range(4):
        cp_in[i].wait()
        rows = dot(dv[...], cp[:, i * 256 : (i + 1) * 256])
        dt[i * 256 : (i + 1) * 256, own_cols] = rows.T.astype(BF16)
        if i % 2:
            h = i // 2
            z_own_dn.append(send(block(gy, h), block(gy, h), z_up, block(group(x, down(z)), h)))
            z_own_up.append(send(block(gy, h), block(gy, h), z_dn, block(group(x, up(z)), h)))
            relayed.append(send(block(gy, h), rel.at[h], (x_up, x_dn)[h], rel.at[h]))

    y_other_dn, y_other_up = [], []
    for wait, rows in ((x_lo, low), (x_hi, high)):
        wait()
        y_other_dn.append(relay_piece(other, y_up, slot(1 - xl, down(y), c), rows))
        y_other_up.append(relay_piece(other, y_dn, slot(1 - xl, up(y), c), rows))
        done.append(relay_piece(other, partner, slot(1 - xl, y, 1 - c), rows))
    x_far = []
    for h in range(2):
        relayed[h]()
        origin = group((down(x), up(x))[h], z)
        x_far.append(send(rel.at[h], block(origin, h), (x_up, x_dn)[h], block(group((x + 2) % 4, z), h)))
    y_own_dn()
    far_lo = relay_piece(slot(xl, down(y), c), y_up, slot(xl, (y + 2) % 4, c), low)
    done.append(relay_piece(slot(xl, down(y), c), partner, slot(xl, down(y), 1 - c)))
    y_own_up()
    far_hi = relay_piece(slot(xl, up(y), c), y_dn, slot(xl, (y + 2) % 4, c), high)
    done.append(relay_piece(slot(xl, up(y), c), partner, slot(xl, up(y), 1 - c)))
    z_own_dn[0]()
    b = group(x, down(z))
    done.append(send(block(b, 0), block(b, 0), z_up, block(group(x, (z + 2) % 4), 0)))
    z_own_up[1]()
    b = group(x, up(z))
    done.append(send(block(b, 1), block(b, 1), z_dn, block(group(x, (z + 2) % 4), 1)))
    done += [z_own_dn[1], z_own_up[0]]
    far = (x + 2) % 4
    b = group(far, z)
    z_far_dn, z_far_up = [], []
    for h in range(2):
        x_far[h]()
        z_far_dn.append(send(block(b, h), block(b, h), z_up, block(group(far, down(z)), h)))
        z_far_up.append(send(block(b, h), block(b, h), z_dn, block(group(far, up(z)), h)))
    for wait, rows in ((far_lo, low), (far_hi, high)):
        wait()
        k = slot(xl, (y + 2) % 4, c)
        done.append(relay_piece(k, partner, slot(xl, (y + 2) % 4, 1 - c), rows))
    k = slot(1 - xl, down(y), c)
    y_other_dn[0]()
    far_lo = relay_piece(k, y_up, slot(1 - xl, (y + 2) % 4, c), low)
    done.append(relay_piece(k, partner, slot(1 - xl, down(y), 1 - c), low))
    k = slot(1 - xl, up(y), c)
    y_other_up[1]()
    far_hi = relay_piece(k, y_dn, slot(1 - xl, (y + 2) % 4, c), high)
    done.append(relay_piece(k, partner, slot(1 - xl, up(y), 1 - c), high))
    y_other_dn[1]()
    k = slot(1 - xl, down(y), c)
    done.append(relay_piece(k, partner, slot(1 - xl, down(y), 1 - c), high))
    y_other_up[0]()
    k = slot(1 - xl, up(y), c)
    done.append(relay_piece(k, partner, slot(1 - xl, up(y), 1 - c), low))
    z_far_dn[0]()
    b = group(far, down(z))
    done.append(send(block(b, 0), block(b, 0), z_up, block(group(far, (z + 2) % 4), 0)))
    z_far_up[1]()
    b = group(far, up(z))
    done.append(send(block(b, 1), block(b, 1), z_dn, block(group(far, (z + 2) % 4), 1)))
    done += [z_far_dn[1], z_far_up[0]]
    for wait, rows in ((far_lo, low), (far_hi, high)):
        wait()
        k = slot(1 - xl, (y + 2) % 4, c)
        done.append(relay_piece(k, partner, slot(1 - xl, (y + 2) % 4, 1 - c), rows))
    own_in.wait()
    z_in.wait()
    for wait in done:
        wait()

    @pl.loop(0, 8)
    def _(i):
        cols = pl.ds(pl.multiple_of(i * 256, 256), 256)
        m = dot(dt[...], cq[:, cols])
        zw[:, cols] = (zw[:, cols].astype(F32) * m).astype(BF16)

    for copy in sent:
        copy.wait_send()
    gathered = len(sent)

    @pl.loop(0, 8)
    def _(g):
        rows = pl.ds(pl.multiple_of(g * ROWS, ROWS), ROWS)
        u = lax.dot_general(zw[...], cq[rows, :], (((1,), (1,)), ((), ())), preferred_element_type=F32).astype(BF16)
        gz, gh = g // 2, g % 2
        for t, start in enumerate((gh * 512 + gz * 128, 1024 + g * 128, 2048 + g * 128)):
            dt[:, pl.ds(pl.multiple_of(start, PIECE), PIECE)] = u[:, t * PIECE : (t + 1) * PIECE]

    def lhs(core, xs):
        parts = [cp[pl.ds(pl.multiple_of(b * ROWS + core * CORE_ROWS, CORE_ROWS), CORE_ROWS), :] for b in xs]
        return jnp.concatenate(parts, axis=0)

    def chunk(t, r, core):
        if t == 0:
            to = (x + r) % 4
            v = dot(lhs(core, [(to % 2) * 4 + b for b in range(4)]), dt[:, pl.ds(pl.multiple_of((to // 2) * 512, 512), 512)])
            where = [(b, cc) for b in range(4) for cc in range(4)]
        elif t == 1:
            to = (y + r) % 4
            v = dot(lhs(core, [to, 4 + to]), dt[:, 1024:2048])
            where = [(xx % 2, zz * 2 + xx // 2) for zz in range(4) for xx in range(4)]
        else:
            to = (z + r) % 4
            v = dot(lhs(core, range(8)), dt[:, pl.ds(pl.multiple_of(2048 + to * 256, 256), 256)])
            where = [((xx % 2) * 4 + yy, xx // 2) for xx in range(4) for yy in range(4)]
        return [v[a * CORE_ROWS : (a + 1) * CORE_ROWS, b * PIECE : (b + 1) * PIECE] for a, b in where]

    ups, downs = (x_up, y_up, z_up), (x_dn, y_dn, z_dn)
    place = (x, y, z)
    steps = [(r, t) for r in (2, 1, 3, 0) for t in range(3)]
    index = {s: i for i, s in enumerate(steps)}

    def part(ref, i, start, size):
        return ref.at[pl.ds(start, size), i * PIECE : (i + 1) * PIECE]

    crossed, arrive = {}, {}

    def give(r, t):
        i = index[r, t]
        for b, v in enumerate(chunk(t, r, 1 - c)):
            cq[b * CORE_ROWS : (b + 1) * CORE_ROWS, i * PIECE : (i + 1) * PIECE] = v.astype(BF16)
        crossed[i] = send(part(cq, i, 0, NBF), part(dr, i, 0, NBF), partner, part(dr, i, 0, NBF))

    def keep(r, t):
        i = index[r, t]
        values = chunk(t, r, c)
        crossed[i]()
        for b, v in enumerate(values):
            at = (slice(b * CORE_ROWS, (b + 1) * CORE_ROWS), slice(i * PIECE, (i + 1) * PIECE))
            dr[at] = (v + dr[at].astype(F32)).astype(BF16)
        if r == 2:
            arrive["in", 0, t] = send(part(dr, i, 0, HALF), part(rin1, t, 0, HALF), ups[t], part(rin1, t, 0, HALF))
            arrive["in", 1, t] = send(part(dr, i, HALF, HALF), part(rin1, t, HALF, HALF), downs[t], part(rin1, t, HALF, HALF))
        elif r == 1:
            arrive["up", 1, t] = send(part(dr, i, HALF, HALF), part(rf1, t, HALF, HALF), ups[t], part(rf1, t, HALF, HALF))
        elif r == 3:
            arrive["dn", 0, t] = send(part(dr, i, 0, HALF), part(rf1, 3 + t, 0, HALF), downs[t], part(rf1, 3 + t, 0, HALF))

    def pass_on(side, t):
        r, h = ((1, 0), (3, 1))[side]
        i = index[r, t]
        arrive["in", h, t]()
        rows = slice(h * HALF, (h + 1) * HALF)
        at = (rows, slice(i * PIECE, (i + 1) * PIECE))
        dr[at] = (dr[at].astype(F32) + rin1[rows, t * PIECE : (t + 1) * PIECE].astype(F32)).astype(BF16)
        to, k = ((ups[t], t), (downs[t], 3 + t))[side]
        arrive[("up", "dn")[side], h, t] = send(part(dr, i, h * HALF, HALF), part(rf1, k, h * HALF, HALF), to, part(rf1, k, h * HALF, HALF))

    give(*steps[0])
    for n, step in enumerate(steps):
        if n + 1 < len(steps):
            give(*steps[n + 1])
        keep(*step)
        if n == 8:
            for t in range(3):
                pass_on(0, t)
    for t in range(3):
        pass_on(1, t)
    for t in range(3):
        for h in range(2):
            arrive["up", h, t]()
            arrive["dn", h, t]()

    def value1(t, start, size):
        i = index[0, t]
        rows = pl.ds(start, size)
        total = dr[rows, i * PIECE : (i + 1) * PIECE].astype(F32)
        for k in (t, 3 + t):
            total += rf1[rows, k * PIECE : (k + 1) * PIECE].astype(F32)
        return total

    def ring(axes, size, value, rin, rf, base):
        half = size // 2
        got = {}
        for t in range(3):
            a, i = axes[t], index[0, t]
            to = ups[a], downs[a]
            far = (place[a] + 2) % 4 * size

            def put(offset, n, v, i=i, t=t):
                start = pl.multiple_of(base[t] + offset, 32)
                dr[pl.ds(start, n), i * PIECE : (i + 1) * PIECE] = v.astype(BF16)
                return part(dr, i, start, n)

            far_part = put(far, size, value(t, far, size))
            start = pl.multiple_of(base[t] + far, 32)
            del far_part
            for h in range(2):
                got["in", h, t] = send(part(dr, i, pl.multiple_of(start + h * half, 32), half), part(rin, t, h * half, half), to[h], part(rin, t, h * half, half))
            for side, near in ((0, up(place[a])), (1, down(place[a]))):
                h = 1 - side
                at = pl.multiple_of(near * size + h * half, 32)
                src = put(at, half, value(t, at, half))
                got[side, h, t] = send(src, part(rf, side * 3 + t, h * half, half), to[side], part(rf, side * 3 + t, h * half, half))
        for t in range(3):
            a, i = axes[t], index[0, t]
            to = ups[a], downs[a]
            for side, near in ((0, up(place[a])), (1, down(place[a]))):
                h = side
                at = pl.multiple_of(near * size + h * half, 32)
                v = value(t, at, half)
                got["in", h, t]()
                v += rin[h * half : (h + 1) * half, t * PIECE : (t + 1) * PIECE].astype(F32)
                start = pl.multiple_of(base[t] + at, 32)
                dr[pl.ds(start, half), i * PIECE : (i + 1) * PIECE] = v.astype(BF16)
                got[side, h, t] = send(part(dr, i, start, half), part(rf, side * 3 + t, h * half, half), to[side], part(rf, side * 3 + t, h * half, half))
        for t in range(3):
            for side in range(2):
                for h in range(2):
                    got[side, h, t]()

    second, third = (1, 2, 0), (2, 0, 1)
    ring(second, 768, value1, rin2, rf2, (0, 0, 0))
    base2 = [place[second[t]] * 768 for t in range(3)]

    def value2(t, offset, size):
        total = value1(t, pl.multiple_of(base2[t] + offset, 32), size)
        for k in (t, 3 + t):
            total += rf2[pl.ds(offset, size), k * PIECE : (k + 1) * PIECE].astype(F32)
        return total

    ring(third, 192, value2, rin3, rf3, base2)
    for t in range(3):
        total = value2(t, pl.multiple_of(place[third[t]] * CORE_ROWS, 32), CORE_ROWS)
        for k in (t, 3 + t):
            total += rf3[:, k * PIECE : (k + 1) * PIECE].astype(F32)
        out_ref[:, t * PIECE : (t + 1) * PIECE] = total

    for copy in sent[gathered:]:
        copy.wait_send()


def local(collocation, density, kernel_values):
    coefficients = kernel_values.reshape(PANEL, NQ)
    return pl.pallas_call(
        kernel,
        out_shape=jax.ShapeDtypeStruct((CORE_ROWS, ROWS), F32),
        in_specs=[pl.BlockSpec(memory_space=pl.ANY)] * 3,
        out_specs=pl.BlockSpec(memory_space=pltpu.VMEM),
        scratch_shapes=[
            pltpu.VMEM((NBF, PANEL), BF16),
            pltpu.VMEM((ROWS, NBF), BF16),
            pltpu.VMEM((PANEL, NBF), BF16),
            pltpu.VMEM((NBF, NQ), BF16),
            pltpu.VMEM((PANEL, NQ), BF16),
            pltpu.VMEM((2, 512, ROWS), BF16),
            pltpu.VMEM((NBF, 12 * PIECE), BF16),
            pltpu.VMEM((NBF, 3 * PIECE), BF16),
            pltpu.VMEM((NBF, 6 * PIECE), BF16),
            pltpu.VMEM((768, 3 * PIECE), BF16),
            pltpu.VMEM((768, 6 * PIECE), BF16),
            pltpu.VMEM((192, 3 * PIECE), BF16),
            pltpu.VMEM((192, 6 * PIECE), BF16),
            pltpu.SemaphoreType.DMA((N_SENDS,)),
            pltpu.SemaphoreType.DMA((N_SENDS,)),
            pltpu.SemaphoreType.DMA((8,)),
        ],
        compiler_params=pltpu.CompilerParams(
            collective_id=0, has_side_effects=True, vmem_limit_bytes=67043328
        ),
    )(collocation, density, coefficients)


def solution(mesh):
    return jax.shard_map(
        local,
        mesh=mesh,
        in_specs=(P(None, "gx"), P("gy", None), P("gx", None, "gy", None)),
        out_specs=P("gx", "gy"),
        check_vma=False,
    )
```

```python
import jax
import jax.numpy as jnp
from jax import lax
from jax.experimental import pallas as pl
from jax.experimental.pallas import tpu as pltpu
from jax.sharding import PartitionSpec as P

MESH = pl.DeviceIdType.MESH
BF16 = jnp.bfloat16
F32 = jnp.float32

NBF = 3072
PANEL = 1024
PIECE = 128
ROWS = 384
NQ = 2048
HALF = NBF // 2
CORE_ROWS = 192
N_SENDS = 128


def dot(a, b):
    return jnp.dot(a, b, preferred_element_type=F32)


def kernel(
    c_ref, d_ref, z_ref, out_ref,
    cp, dv, dt, cq, zw, zf, rel, gv, ow, dr, rin1, rf1, rin2, rf2, rin3, rf3,
    send_sem, recv_sem, local_sem,
):
    gx, gy = lax.axis_index("gx"), lax.axis_index("gy")
    c, y, xl = gx % 2, (gx // 2) % 4, gx // 8
    z, xh = gy // 2, gy % 2
    x = xh * 2 + xl

    def device(x, y, z, c):
        return {"gx": ((x % 2) * 4 + y) * 2 + c, "gy": z * 2 + x // 2}

    def up(v):
        return (v + 1) % 4

    def down(v):
        return (v + 3) % 4

    partner = device(x, y, z, 1 - c)
    x_up, x_dn = device(up(x), y, z, c), device(down(x), y, z, c)
    y_up, y_dn = device(x, up(y), z, c), device(x, down(y), z, c)
    z_up, z_dn = device(x, y, up(z), c), device(x, y, down(z), c)

    barrier = pltpu.get_barrier_semaphore()
    neighbours = (partner, x_up, x_dn, y_up, y_dn, z_up, z_dn)
    for one in neighbours:
        pl.semaphore_signal(barrier, inc=1, device_id=one, device_id_type=MESH)

    locals_ = []

    def fetch(src, dst):
        copy = pltpu.make_async_copy(src, dst, local_sem.at[len(locals_)])
        copy.start()
        locals_.append(copy)
        return copy

    def column(ref, k, rows=None, width=PIECE):
        cols = pl.ds(pl.multiple_of(k * width, PIECE), width)
        return ref.at[:, cols] if rows is None else ref.at[pl.ds(*rows), cols]

    d_in = fetch(d_ref, dv)
    cp_in = [fetch(column(c_ref, i, width=256), column(cp, i, width=256)) for i in range(4)]
    own_in = fetch(column(c_ref, gy), column(cq, gx))
    z_in = []
    for i in range(6):
        ref, rows = (gv, ow)[i // 4], min(NBF, PANEL * 16 - i * NBF)
        z_in.append(fetch(z_ref.at[pl.ds(i * NBF, rows)], column(ref, i % 4, (0, rows))))
    pl.semaphore_wait(barrier, len(neighbours))

    sent = []

    def send(src, dst, to, lands):
        i = len(sent)
        copy = pltpu.make_async_remote_copy(
            src_ref=src, dst_ref=dst, send_sem=send_sem.at[i], recv_sem=recv_sem.at[i],
            device_id=to, device_id_type=MESH,
        )
        copy.start()
        sent.append(copy)
        arrival = pltpu.make_async_remote_copy(
            src_ref=lands, dst_ref=lands, send_sem=send_sem.at[i], recv_sem=recv_sem.at[i],
            device_id=to, device_id_type=MESH,
        )
        return arrival.wait_recv

    def slot(xl, y, c):
        return (xl * 4 + y) * 2 + c

    low, high = (0, HALF), (HALF, HALF)

    def piece(k, rows=None):
        return column(cq, k, rows)

    def relay_piece(k, to, mine, rows=None):
        return send(piece(k, rows), piece(k, rows), to, piece(mine, rows))

    own = column(c_ref, gy)
    y_own_dn = send(own, piece(gx), y_up, piece(slot(xl, down(y), c)))
    y_own_up = send(own, piece(gx), y_dn, piece(slot(xl, up(y), c)))
    other = slot(1 - xl, y, c)
    x_lo = send(column(c_ref, z * 2 + up(x) // 2, low), piece(gx, low), x_up, piece(other, low))
    x_hi = send(column(c_ref, z * 2 + down(x) // 2, high), piece(gx, high), x_dn, piece(other, high))
    near = [send(own, piece(gx), partner, piece(slot(xl, y, 1 - c)))]

    def block(j, q):
        return dt.at[pl.ds(q * 256, 256), pl.ds(pl.multiple_of(j * ROWS, PIECE), ROWS)]

    def group(x, z):
        return z * 2 + x // 2

    def both(j, q, xz):
        return (
            send(block(j, q), block(j, q), z_up, block(group(xz, down(z)), q)),
            send(block(j, q), block(j, q), z_dn, block(group(xz, up(z)), q)),
        )

    def onward(q, xz):
        b = block(group(xz, (down(z), up(z))[q % 2]), q)
        return send(b, b, (z_up, z_dn)[q % 2], block(group(xz, (z + 2) % 4), q))

    own_cols = pl.ds(pl.multiple_of(gy * ROWS, PIECE), ROWS)
    d_in.wait()
    z_own, relayed = [], []
    for q in range(4):
        cp_in[q].wait()
        with jax.named_scope(f"own{q}"):
            rows = dot(dv[...], cp[:, q * 256 : (q + 1) * 256])
            dt[q * 256 : (q + 1) * 256, own_cols] = rows.T.astype(BF16)
        z_own.append(both(gy, q, x))
        relayed.append(send(block(gy, q), rel.at[q], (x_up, x_dn)[q % 2], rel.at[q]))

    def unpack(i):
        ref, n = (gv, ow)[i // 4], min(CORE_ROWS, PANEL - i * CORE_ROWS)
        z_in[i].wait()

        @pl.loop(0, n // 64)
        def _(b):
            with jax.named_scope("unpack"):
                first = pl.multiple_of(b * 1024, 1024)
                zf[...] = ref[pl.ds(first, 1024), (i % 4) * PIECE : (i % 4 + 1) * PIECE].astype(F32)
                to = pl.ds(pl.multiple_of(i * CORE_ROWS + b * 64, 64), 64)
                for k in range(16):
                    zw[to, k * PIECE : (k + 1) * PIECE] = zf[pl.ds(k, 64, stride=16), :].astype(BF16)

    x_far, z_far, next_own, next_far = {}, {}, {}, {}
    far = (x + 2) % 4

    def forward(q):
        relayed[q]()
        origin = group((down(x), up(x))[q % 2], z)
        x_far[q] = send(rel.at[q], block(origin, q), (x_up, x_dn)[q % 2], block(group(far, z), q))

    unpack(0)
    y_other = []
    for wait, rows in ((x_lo, low), (x_hi, high)):
        wait()
        k = other
        y_other.append((
            relay_piece(k, y_up, slot(1 - xl, down(y), c), rows),
            relay_piece(k, y_dn, slot(1 - xl, up(y), c), rows),
        ))
        near.append(relay_piece(k, partner, slot(1 - xl, y, 1 - c), rows))
    forward(0)
    forward(1)
    unpack(1)
    z_own[0][0]()
    next_own[0] = onward(0, x)
    z_own[1][1]()
    next_own[1] = onward(1, x)
    for q in range(2):
        x_far[q]()
        z_far[q] = both(group(far, z), q, far)
    y_own_dn()
    far_lo = relay_piece(slot(xl, down(y), c), y_up, slot(xl, (y + 2) % 4, c), low)
    near.append(relay_piece(slot(xl, down(y), c), partner, slot(xl, down(y), 1 - c)))
    y_own_up()
    far_hi = relay_piece(slot(xl, up(y), c), y_dn, slot(xl, (y + 2) % 4, c), high)
    near.append(relay_piece(slot(xl, up(y), c), partner, slot(xl, up(y), 1 - c)))
    forward(2)
    forward(3)
    unpack(2)
    z_far[0][0]()
    next_far[0] = onward(0, far)
    z_far[1][1]()
    next_far[1] = onward(1, far)
    z_own[2][0]()
    next_own[2] = onward(2, x)
    z_own[3][1]()
    next_own[3] = onward(3, x)
    for q in range(2, 4):
        x_far[q]()
        z_far[q] = both(group(far, z), q, far)
    unpack(3)
    unpack(4)
    unpack(5)

    def m(h, s):
        cols = pl.ds(pl.multiple_of(s * 256, 256), 256)
        rows = pl.ds(h * 512, 512)
        with jax.named_scope(f"m{h}"):
            zw[rows, cols] = (zw[rows, cols].astype(F32) * dot(dt[rows, :], cq[:, cols])).astype(BF16)

    own_in.wait()
    for wait in near:
        wait()
    for wait in (z_own[0][1], z_own[1][0], z_far[0][1], z_far[1][0], next_own[0], next_own[1], next_far[0], next_far[1]):
        wait()

    @pl.loop(0, 2)
    def _(i):
        m(0, (xl + i) % 2 * 4 + y)

    passed = []
    for wait, rows in ((far_lo, low), (far_hi, high)):
        wait()
        k = slot(xl, (y + 2) % 4, c)
        passed.append(relay_piece(k, partner, slot(xl, (y + 2) % 4, 1 - c), rows))
    k = slot(1 - xl, down(y), c)
    y_other[0][0]()
    far_lo = relay_piece(k, y_up, slot(1 - xl, (y + 2) % 4, c), low)
    passed.append(relay_piece(k, partner, slot(1 - xl, down(y), 1 - c), low))
    k = slot(1 - xl, up(y), c)
    y_other[1][1]()
    far_hi = relay_piece(k, y_dn, slot(1 - xl, (y + 2) % 4, c), high)
    passed.append(relay_piece(k, partner, slot(1 - xl, up(y), 1 - c), high))
    z_far[2][0]()
    next_far[2] = onward(2, far)
    z_far[3][1]()
    next_far[3] = onward(3, far)
    y_other[1][0]()
    k = slot(1 - xl, down(y), c)
    passed.append(relay_piece(k, partner, slot(1 - xl, down(y), 1 - c), high))
    y_other[0][1]()
    k = slot(1 - xl, up(y), c)
    passed.append(relay_piece(k, partner, slot(1 - xl, up(y), 1 - c), low))

    @pl.loop(0, 2)
    def _(i):
        m(0, xl * 4 + (y + 1 + 2 * i) % 4)

    for wait in passed:
        wait()

    @pl.loop(0, 3)
    def _(i):
        m(0, jnp.where(i < 2, (1 - xl) * 4 + (y + 1 + 2 * i) % 4, xl * 4 + (y + 2) % 4))

    passed = []
    for wait, rows in ((far_lo, low), (far_hi, high)):
        wait()
        k = slot(1 - xl, (y + 2) % 4, c)
        passed.append(relay_piece(k, partner, slot(1 - xl, (y + 2) % 4, 1 - c), rows))
    for wait in (z_own[2][1], z_own[3][0], z_far[2][1], z_far[3][0], next_own[2], next_own[3], next_far[2], next_far[3], *passed):
        wait()
    m(0, (1 - xl) * 4 + (y + 2) % 4)

    @pl.loop(0, 8)
    def _(s):
        m(1, s)

    for copy in sent:
        copy.wait_send()
    gathered = len(sent)

    def u(t, first, second, col):
        rows = [cq[pl.ds(pl.multiple_of(g * ROWS + t * PIECE, PIECE), PIECE), :] for g in (first, second)]
        with jax.named_scope("u"):
            v = lax.dot_general(
                zw[...], jnp.concatenate(rows, axis=0), (((1,), (1,)), ((), ())), preferred_element_type=F32
            )
            dt[:, pl.ds(pl.multiple_of(col, 256), 256)] = v.astype(BF16)

    def u0(xh):
        @pl.loop(0, 2)
        def _(p):
            u(0, 4 * p + xh, 4 * p + 2 + xh, xh * 512 + p * 256)

    def u1():
        @pl.loop(0, 4)
        def _(p):
            u(1, 2 * p, 2 * p + 1, 1024 + p * 256)

    def u2(first):
        @pl.loop(0, 2)
        def _(p):
            zz = (first - p) % 4
            u(2, 2 * zz, 2 * zz + 1, 2048 + zz * 256)

    def lhs(first, second):
        parts = [
            cp[pl.ds(pl.multiple_of(b * ROWS + core * CORE_ROWS, CORE_ROWS), CORE_ROWS), :]
            for core in (1 - c, c) for b in (first, second)
        ]
        return jnp.concatenate(parts, axis=0)

    def store(v, row, col, where, k):
        for p, ref in enumerate((gv, ow)):
            at = pl.ds(pl.multiple_of(where * CORE_ROWS, CORE_ROWS), CORE_ROWS)
            r = p * 384 + row * CORE_ROWS
            ref[at, k * PIECE : (k + 1) * PIECE] = v[r : r + CORE_ROWS, col * PIECE : (col + 1) * PIECE].astype(BF16)

    def k0(r, k):
        to = (x + r) % 4

        @pl.loop(0, 2)
        def _(n):
            with jax.named_scope("k0"):
                first = (to % 2) * 4 + 2 * n
                v = dot(lhs(first, first + 1), dt[:, pl.ds(pl.multiple_of((to // 2) * 512, 512), 512)])
                for b in range(2):
                    for zz in range(4):
                        store(v, b, zz, (2 * n + b) * 4 + zz, k)

    def k1(r, k):
        to = (y + r) % 4

        @pl.loop(0, 2)
        def _(n):
            with jax.named_scope("k1"):
                v = dot(lhs(to, 4 + to), dt[:, pl.ds(pl.multiple_of(1024 + n * 512, 512), 512)])
                for b in range(2):
                    for zz in range(2):
                        for hh in range(2):
                            store(v, b, zz * 2 + hh, (2 * n + zz) * 4 + hh * 2 + b, k)

    def k2(ra, rb, ka, kb):
        za, zb = (z + ra) % 4, (z + rb) % 4

        @pl.loop(0, 4)
        def _(n):
            with jax.named_scope("k2"):
                rhs = [dt[:, pl.ds(pl.multiple_of(2048 + zz * 256, 256), 256)] for zz in (za, zb)]
                v = dot(lhs(2 * n, 2 * n + 1), jnp.concatenate(rhs, axis=1))
                for i, k in enumerate((ka, kb)):
                    for b in range(2):
                        for hh in range(2):
                            store(v, b, i * 2 + hh, (hh * 2 + n // 2) * 4 + (n % 2) * 2 + b, k)

    ups, downs = (x_up, y_up, z_up), (x_dn, y_dn, z_dn)
    place = (x, y, z)
    steps = [(r, t) for r in (2, 1, 3, 0) for t in range(3)]
    index = {s: i for i, s in enumerate(steps)}

    def part(ref, i, start, size):
        return ref.at[pl.ds(start, size), i * PIECE : (i + 1) * PIECE]

    crossed, arrive, held, free = {}, {}, {}, [None] * 4

    def take():
        k = take.next
        take.next = (k + 1) % 4
        if free[k] is not None:
            sent[free[k]].wait_send()
            waited.add(free[k])
        return k

    take.next, waited = 0, set()

    def give(*chunks):
        ks = [take() for _ in chunks]
        t = chunks[0][1]
        if t == 2:
            k2(chunks[0][0], chunks[1][0], *ks)
        else:
            (k0, k1)[t](chunks[0][0], ks[0])
        for (r, t), k in zip(chunks, ks):
            i = index[r, t]
            held[i], free[k] = k, len(sent)
            crossed[i] = send(part(gv, k, 0, NBF), part(dr, i, 0, NBF), partner, part(dr, i, 0, NBF))

    def keep(*chunks):
        for r, t in chunks:
            i = index[r, t]
            crossed[i]()
            k = held[i]

            @pl.loop(0, 4)
            def _(b, i=i, k=k):
                rows = pl.ds(pl.multiple_of(b * 768, 768), 768)
                at = (rows, slice(i * PIECE, (i + 1) * PIECE))
                dr[at] = (ow[rows, k * PIECE : (k + 1) * PIECE].astype(F32) + dr[at].astype(F32)).astype(BF16)

            if r == 2:
                arrive["in", 0, t] = send(part(dr, i, 0, HALF), part(rin1, t, 0, HALF), ups[t], part(rin1, t, 0, HALF))
                arrive["in", 1, t] = send(part(dr, i, HALF, HALF), part(rin1, t, HALF, HALF), downs[t], part(rin1, t, HALF, HALF))
            elif r == 1:
                arrive["up", 1, t] = send(part(dr, i, HALF, HALF), part(rf1, t, HALF, HALF), ups[t], part(rf1, t, HALF, HALF))
            elif r == 3:
                arrive["dn", 0, t] = send(part(dr, i, 0, HALF), part(rf1, 3 + t, 0, HALF), downs[t], part(rf1, 3 + t, 0, HALF))

    def pass_on(side, t):
        r, h = ((1, 0), (3, 1))[side]
        i = index[r, t]
        arrive["in", h, t]()

        @pl.loop(0, 2)
        def _(b):
            rows = pl.ds(pl.multiple_of(h * HALF + b * 768, 768), 768)
            at = (rows, slice(i * PIECE, (i + 1) * PIECE))
            dr[at] = (dr[at].astype(F32) + rin1[rows, t * PIECE : (t + 1) * PIECE].astype(F32)).astype(BF16)

        to, k = ((ups[t], t), (downs[t], 3 + t))[side]
        arrive[("up", "dn")[side], h, t] = send(part(dr, i, h * HALF, HALF), part(rf1, k, h * HALF, HALF), to, part(rf1, k, h * HALF, HALF))

    u1()
    give((2, 1))
    u0(1 - xh)
    give((2, 0))
    keep((2, 1))
    u2(z + 2)
    give((2, 2), (1, 2))
    keep((2, 0))
    u0(xh)
    give((1, 0))
    keep((2, 2), (1, 2))
    give((1, 1))
    keep((1, 0))
    give((3, 1))
    keep((1, 1))
    pass_on(0, 1)
    give((3, 0))
    keep((3, 1))
    pass_on(1, 1)
    pass_on(0, 0)
    u2(z)
    give((3, 2), (0, 2))
    keep((3, 0))
    pass_on(1, 0)
    pass_on(0, 2)
    give((0, 0))
    keep((3, 2), (0, 2))
    pass_on(1, 2)
    give((0, 1))
    keep((0, 0))
    keep((0, 1))
    for t in range(3):
        for h in range(2):
            arrive["up", h, t]()
            arrive["dn", h, t]()

    def value1(t, start, size):
        i = index[0, t]
        rows = pl.ds(start, size)
        total = dr[rows, i * PIECE : (i + 1) * PIECE].astype(F32)
        for k in (t, 3 + t):
            total += rf1[rows, k * PIECE : (k + 1) * PIECE].astype(F32)
        return total

    def ring(axes, size, value, rin, rf, base):
        half = size // 2
        got = {}
        for t in range(3):
            a, i = axes[t], index[0, t]
            to = ups[a], downs[a]
            far = (place[a] + 2) % 4 * size

            def put(offset, n, v, i=i, t=t):
                start = pl.multiple_of(base[t] + offset, 32)
                dr[pl.ds(start, n), i * PIECE : (i + 1) * PIECE] = v.astype(BF16)
                return part(dr, i, start, n)

            far_part = put(far, size, value(t, far, size))
            start = pl.multiple_of(base[t] + far, 32)
            del far_part
            for h in range(2):
                got["in", h, t] = send(part(dr, i, pl.multiple_of(start + h * half, 32), half), part(rin, t, h * half, half), to[h], part(rin, t, h * half, half))
            for side, near in ((0, up(place[a])), (1, down(place[a]))):
                h = 1 - side
                at = pl.multiple_of(near * size + h * half, 32)
                src = put(at, half, value(t, at, half))
                got[side, h, t] = send(src, part(rf, side * 3 + t, h * half, half), to[side], part(rf, side * 3 + t, h * half, half))
        for t in range(3):
            a, i = axes[t], index[0, t]
            to = ups[a], downs[a]
            for side, near in ((0, up(place[a])), (1, down(place[a]))):
                h = side
                at = pl.multiple_of(near * size + h * half, 32)
                v = value(t, at, half)
                got["in", h, t]()
                v += rin[h * half : (h + 1) * half, t * PIECE : (t + 1) * PIECE].astype(F32)
                start = pl.multiple_of(base[t] + at, 32)
                dr[pl.ds(start, half), i * PIECE : (i + 1) * PIECE] = v.astype(BF16)
                got[side, h, t] = send(part(dr, i, start, half), part(rf, side * 3 + t, h * half, half), to[side], part(rf, side * 3 + t, h * half, half))
        for t in range(3):
            for side in range(2):
                for h in range(2):
                    got[side, h, t]()

    second, third = (1, 2, 0), (2, 0, 1)
    ring(second, 768, value1, rin2, rf2, (0, 0, 0))
    base2 = [place[second[t]] * 768 for t in range(3)]

    def value2(t, offset, size):
        total = value1(t, pl.multiple_of(base2[t] + offset, 32), size)
        for k in (t, 3 + t):
            total += rf2[pl.ds(offset, size), k * PIECE : (k + 1) * PIECE].astype(F32)
        return total

    ring(third, 192, value2, rin3, rf3, base2)
    for t in range(3):
        total = value2(t, pl.multiple_of(place[third[t]] * CORE_ROWS, 32), CORE_ROWS)
        for k in (t, 3 + t):
            total += rf3[:, k * PIECE : (k + 1) * PIECE].astype(F32)
        out_ref[:, t * PIECE : (t + 1) * PIECE] = total

    for i in range(gathered, len(sent)):
        if i not in waited:
            sent[i].wait_send()


def local(collocation, density, kernel_values):
    coefficients = kernel_values.reshape(PANEL * 16, PIECE)
    return pl.pallas_call(
        kernel,
        out_shape=jax.ShapeDtypeStruct((CORE_ROWS, ROWS), F32),
        in_specs=[pl.BlockSpec(memory_space=pl.ANY)] * 3,
        out_specs=pl.BlockSpec(memory_space=pltpu.VMEM),
        scratch_shapes=[
            pltpu.VMEM((NBF, PANEL), BF16),
            pltpu.VMEM((ROWS, NBF), BF16),
            pltpu.VMEM((PANEL, NBF), BF16),
            pltpu.VMEM((NBF, NQ), BF16),
            pltpu.VMEM((PANEL, NQ), BF16),
            pltpu.VMEM((1024, PIECE), F32),
            pltpu.VMEM((4, 256, ROWS), BF16),
            pltpu.VMEM((NBF, 4 * PIECE), BF16),
            pltpu.VMEM((NBF, 4 * PIECE), BF16),
            pltpu.VMEM((NBF, 12 * PIECE), BF16),
            pltpu.VMEM((NBF, 3 * PIECE), BF16),
            pltpu.VMEM((NBF, 6 * PIECE), BF16),
            pltpu.VMEM((768, 3 * PIECE), BF16),
            pltpu.VMEM((768, 6 * PIECE), BF16),
            pltpu.VMEM((192, 3 * PIECE), BF16),
            pltpu.VMEM((192, 6 * PIECE), BF16),
            pltpu.SemaphoreType.DMA((N_SENDS,)),
            pltpu.SemaphoreType.DMA((N_SENDS,)),
            pltpu.SemaphoreType.DMA((12,)),
        ],
        compiler_params=pltpu.CompilerParams(
            collective_id=0, has_side_effects=True, vmem_limit_bytes=67043328
        ),
    )(collocation, density, coefficients)


def solution(mesh):
    return jax.shard_map(
        local,
        mesh=mesh,
        in_specs=(P(None, "gx"), P("gy", None), P("gx", None, "gy", None)),
        out_specs=P("gx", "gy"),
        check_vma=False,
    )
```

```python
import jax
import jax.numpy as jnp
from jax import lax
from jax.experimental import pallas as pl
from jax.experimental.pallas import tpu as pltpu
from jax.sharding import PartitionSpec as P

MESH = pl.DeviceIdType.MESH
BF16 = jnp.bfloat16
F32 = jnp.float32

NBF = 3072
PANEL = 1024
PIECE = 128
ROWS = 384
NQ = 2048
HALF = NBF // 2
CORE_ROWS = 192
N_SENDS = 128


def dot(a, b):
    return jnp.dot(a, b, preferred_element_type=F32)


def kernel(
    c_ref, d_ref, z_ref, out_ref,
    cp, dv, dt, cq, zw, acc, zf, rel, gv, ow, dr, uin, uf, rin1, rf1, rin2, rf2, rin3, rf3,
    send_sem, recv_sem, local_sem,
):
    gx, gy = lax.axis_index("gx"), lax.axis_index("gy")
    c, y, xl = gx % 2, (gx // 2) % 4, gx // 8
    z, xh = gy // 2, gy % 2
    x = xh * 2 + xl

    def device(x, y, z, c):
        return {"gx": ((x % 2) * 4 + y) * 2 + c, "gy": z * 2 + x // 2}

    def up(v):
        return (v + 1) % 4

    def down(v):
        return (v + 3) % 4

    partner = device(x, y, z, 1 - c)
    x_up, x_dn = device(up(x), y, z, c), device(down(x), y, z, c)
    y_up, y_dn = device(x, up(y), z, c), device(x, down(y), z, c)
    z_up, z_dn = device(x, y, up(z), c), device(x, y, down(z), c)

    barrier = pltpu.get_barrier_semaphore()
    neighbours = (partner, x_up, x_dn, y_up, y_dn, z_up, z_dn)
    for one in neighbours:
        pl.semaphore_signal(barrier, inc=1, device_id=one, device_id_type=MESH)

    locals_ = []

    def fetch(src, dst):
        copy = pltpu.make_async_copy(src, dst, local_sem.at[len(locals_)])
        copy.start()
        locals_.append(copy)
        return copy

    def column(ref, k, rows=None, width=PIECE):
        cols = pl.ds(pl.multiple_of(k * width, PIECE), width)
        return ref.at[:, cols] if rows is None else ref.at[pl.ds(*rows), cols]

    d_in = fetch(d_ref, dv)
    cp_in = [fetch(column(c_ref, i, width=256), column(cp, i, width=256)) for i in range(4)]
    own_in = fetch(column(c_ref, gy), column(cq, gx))
    pl.semaphore_wait(barrier, len(neighbours))

    sent = []

    def send(src, dst, to, lands):
        i = len(sent)
        copy = pltpu.make_async_remote_copy(
            src_ref=src, dst_ref=dst, send_sem=send_sem.at[i], recv_sem=recv_sem.at[i],
            device_id=to, device_id_type=MESH,
        )
        copy.start()
        sent.append(copy)
        arrival = pltpu.make_async_remote_copy(
            src_ref=lands, dst_ref=lands, send_sem=send_sem.at[i], recv_sem=recv_sem.at[i],
            device_id=to, device_id_type=MESH,
        )
        return arrival.wait_recv

    def slot(xl, y, c):
        return (xl * 4 + y) * 2 + c

    low, high = (0, HALF), (HALF, HALF)

    def piece(k, rows=None):
        return column(cq, k, rows)

    def relay_piece(k, to, mine, rows=None):
        return send(piece(k, rows), piece(k, rows), to, piece(mine, rows))

    own_in.wait()
    own = piece(gx)
    y_own_dn = send(own, piece(gx), y_up, piece(slot(xl, down(y), c)))
    y_own_up = send(own, piece(gx), y_dn, piece(slot(xl, up(y), c)))
    other = slot(1 - xl, y, c)
    x_lo = send(column(c_ref, z * 2 + up(x) // 2, low), piece(gx, low), x_up, piece(other, low))
    x_hi = send(column(c_ref, z * 2 + down(x) // 2, high), piece(gx, high), x_dn, piece(other, high))
    near = [send(own, piece(gx), partner, piece(slot(xl, y, 1 - c)))]

    def block(j, q):
        return dt.at[pl.ds(q * 256, 256), pl.ds(pl.multiple_of(j * ROWS, PIECE), ROWS)]

    def group(x, z):
        return z * 2 + x // 2

    def both(j, q, xz):
        return (
            send(block(j, q), block(j, q), z_up, block(group(xz, down(z)), q)),
            send(block(j, q), block(j, q), z_dn, block(group(xz, up(z)), q)),
        )

    def onward(q, xz):
        b = block(group(xz, (down(z), up(z))[q % 2]), q)
        return send(b, b, (z_up, z_dn)[q % 2], block(group(xz, (z + 2) % 4), q))

    own_cols = pl.ds(pl.multiple_of(gy * ROWS, PIECE), ROWS)
    d_in.wait()
    z_own, relayed = [], []
    for q in range(4):
        cp_in[q].wait()
        with jax.named_scope(f"own{q}"):
            rows = dot(dv[...], cp[:, q * 256 : (q + 1) * 256])
            dt[q * 256 : (q + 1) * 256, own_cols] = rows.T.astype(BF16)
        z_own.append(both(gy, q, x))
        relayed.append(send(block(gy, q), rel.at[q], (x_up, x_dn)[q % 2], rel.at[q]))

    z_in = []
    for i in range(6):
        ref, rows = (gv, ow)[i // 4], min(NBF, PANEL * 16 - i * NBF)
        z_in.append(fetch(z_ref.at[pl.ds(i * NBF, rows)], column(ref, i % 4, (0, rows))))

    def unpack(i):
        ref, n = (gv, ow)[i // 4], min(CORE_ROWS, PANEL - i * CORE_ROWS)
        z_in[i].wait()

        @pl.loop(0, n // 64)
        def _(b):
            with jax.named_scope("unpack"):
                first = pl.multiple_of(b * 1024, 1024)
                zf[...] = ref[pl.ds(first, 1024), (i % 4) * PIECE : (i % 4 + 1) * PIECE].astype(F32)
                to = pl.ds(pl.multiple_of(i * CORE_ROWS + b * 64, 64), 64)
                for k in range(16):
                    zw[to, k * PIECE : (k + 1) * PIECE] = zf[pl.ds(k, 64, stride=16), :].astype(BF16)

    x_far, z_far, next_own, next_far = {}, {}, {}, {}
    far = (x + 2) % 4

    def forward(q):
        relayed[q]()
        origin = group((down(x), up(x))[q % 2], z)
        x_far[q] = send(rel.at[q], block(origin, q), (x_up, x_dn)[q % 2], block(group(far, z), q))

    unpack(0)
    unpack(1)
    y_other = []
    for wait, rows in ((x_lo, low), (x_hi, high)):
        wait()
        k = other
        y_other.append((
            relay_piece(k, y_up, slot(1 - xl, down(y), c), rows),
            relay_piece(k, y_dn, slot(1 - xl, up(y), c), rows),
        ))
        near.append(relay_piece(k, partner, slot(1 - xl, y, 1 - c), rows))
    z_own[0][0]()
    next_own[0] = onward(0, x)
    z_own[1][1]()
    next_own[1] = onward(1, x)
    forward(0)
    forward(1)
    y_own_dn()
    far_lo = relay_piece(slot(xl, down(y), c), y_up, slot(xl, (y + 2) % 4, c), low)
    near.append(relay_piece(slot(xl, down(y), c), partner, slot(xl, down(y), 1 - c)))
    y_own_up()
    far_hi = relay_piece(slot(xl, up(y), c), y_dn, slot(xl, (y + 2) % 4, c), high)
    near.append(relay_piece(slot(xl, up(y), c), partner, slot(xl, up(y), 1 - c)))
    z_own[2][0]()
    next_own[2] = onward(2, x)
    forward(2)
    forward(3)
    z_own[3][1]()
    next_own[3] = onward(3, x)
    unpack(2)
    for q in range(4):
        x_far[q]()
        z_far[q] = both(group(far, z), q, far)
        if q % 2:
            unpack(3 + q // 2)
    unpack(5)

    def wpart(which, s):
        cols = pl.ds(pl.multiple_of(s * 256, 256), 256)
        near_js = [2 * zz + xh for zz in range(4)]
        far_js = [2 * ((z + i) % 4) + 1 - xh for i in (0, 1, 3)]
        last_js = [2 * ((z + 2) % 4) + 1 - xh]
        js = {"near": near_js, "far": far_js, "last": last_js, "all": near_js + far_js + last_js}[which]
        with jax.named_scope("m" + which):
            at = [pl.ds(pl.multiple_of(j * ROWS, PIECE), ROWS) for j in js]
            if which == "all":
                v = dot(dt[...], cq[:, cols])
            else:
                v = dot(jnp.concatenate([dt[:, a] for a in at], axis=1), jnp.concatenate([cq[a, cols] for a in at], axis=0))
            if which == "near":
                acc[:, cols] = v
            elif which == "far":
                acc[:, cols] += v
            else:
                v = v if which == "all" else v + acc[:, cols]
                zw[:, cols] = (zw[:, cols].astype(F32) * v).astype(BF16)

    for wait in near:
        wait()
    for wait in (z_own[0][1], z_own[1][0], z_own[2][1], z_own[3][0], next_own[0], next_own[1], next_own[2], next_own[3]):
        wait()

    @pl.loop(0, 4)
    def _(i):
        wpart("near", jnp.where(i == 3, (1 - xl) * 4 + y, xl * 4 + (y + i + i // 2) % 4))

    passed = []
    k = slot(1 - xl, down(y), c)
    y_other[0][0]()
    far_other_lo = relay_piece(k, y_up, slot(1 - xl, (y + 2) % 4, c), low)
    passed.append(relay_piece(k, partner, slot(1 - xl, down(y), 1 - c), low))
    k = slot(1 - xl, up(y), c)
    y_other[1][1]()
    far_other_hi = relay_piece(k, y_dn, slot(1 - xl, (y + 2) % 4, c), high)
    passed.append(relay_piece(k, partner, slot(1 - xl, up(y), 1 - c), high))
    z_far[0][0]()
    next_far[0] = onward(0, far)
    y_other[1][0]()
    k = slot(1 - xl, down(y), c)
    passed.append(relay_piece(k, partner, slot(1 - xl, down(y), 1 - c), high))
    y_other[0][1]()
    k = slot(1 - xl, up(y), c)
    passed.append(relay_piece(k, partner, slot(1 - xl, up(y), 1 - c), low))
    z_far[1][1]()
    next_far[1] = onward(1, far)
    for wait in passed:
        wait()

    @pl.loop(0, 2)
    def _(i):
        wpart("near", (1 - xl) * 4 + (y + 1 + 2 * i) % 4)

    z_far[2][0]()
    next_far[2] = onward(2, far)
    passed = []
    for wait, rows in ((far_lo, low), (far_hi, high)):
        wait()
        k = slot(xl, (y + 2) % 4, c)
        passed.append(relay_piece(k, partner, slot(xl, (y + 2) % 4, 1 - c), rows))
    z_far[3][1]()
    next_far[3] = onward(3, far)
    for wait in passed:
        wait()
    wpart("near", xl * 4 + (y + 2) % 4)
    for wait in (z_far[0][1], z_far[1][0], z_far[2][1], z_far[3][0]):
        wait()
    newest = (1 - xl) * 4 + (y + 2) % 4

    @pl.loop(0, 7)
    def _(i):
        wpart("far", (newest + 1 + i) % 8)

    passed = []
    for wait, rows in ((far_other_lo, low), (far_other_hi, high)):
        wait()
        k = slot(1 - xl, (y + 2) % 4, c)
        passed.append(relay_piece(k, partner, slot(1 - xl, (y + 2) % 4, 1 - c), rows))
    for q in range(4):
        next_far[q]()

    @pl.loop(0, 7)
    def _(i):
        wpart("last", (newest + 1 + i) % 8)

    for wait in passed:
        wait()
    wpart("all", newest)

    for copy in sent:
        copy.wait_send()
    gathered = len(sent)

    def u(t, first, second, col):
        rows = [cq[pl.ds(pl.multiple_of(g * ROWS + t * PIECE, PIECE), PIECE), :] for g in (first, second)]
        with jax.named_scope("u"):
            v = lax.dot_general(
                zw[...], jnp.concatenate(rows, axis=0), (((1,), (1,)), ((), ())), preferred_element_type=F32
            )
            dt[:, pl.ds(pl.multiple_of(col, 256), 256)] = v.astype(BF16)

    def u0(xh):
        @pl.loop(0, 2)
        def _(p):
            u(0, 4 * p + xh, 4 * p + 2 + xh, xh * 512 + p * 256)

    def u2(t, first, count):
        @pl.loop(0, count)
        def _(p):
            zz = (first + 2 * p) % 4
            u(t, 2 * zz, 2 * zz + 1, t * 1024 + zz * 256)

    def upart(t, r, h):
        return dt.at[pl.ds(h * 512, 512), pl.ds(pl.multiple_of(t * 1024 + (z + r) % 4 * 256, 256), 256)]

    def uplace(ref, i, h):
        return ref.at[pl.ds(h * 512, 512), i * 256 : (i + 1) * 256]

    moved = {}

    def u_begin(t):
        for h, to in ((0, z_up), (1, z_dn)):
            lands = uplace(uin, t - 1, h)
            moved["in", h, t] = send(upart(t, 2, h), lands, to, lands)

    def u_direct(t):
        for side, r, h, to in ((0, 1, 1, z_up), (1, 3, 0, z_dn)):
            lands = uplace(uf, 2 * side + t - 1, h)
            moved[side, h, t] = send(upart(t, r, h), lands, to, lands)

    def u_pass(t):
        for side, r, h, to in ((0, 1, 0, z_up), (1, 3, 1, z_dn)):
            moved["in", h, t]()
            src = upart(t, r, h)
            src[...] = (src[...].astype(F32) + uplace(uin, t - 1, h)[...].astype(F32)).astype(BF16)
            lands = uplace(uf, 2 * side + t - 1, h)
            moved[side, h, t] = send(src, lands, to, lands)

    def u_end(t):
        for h in range(2):
            moved[0, h, t]()
            moved[1, h, t]()
            src = upart(t, 0, h)
            total = src[...].astype(F32)
            for side in range(2):
                total += uplace(uf, 2 * side + t - 1, h)[...].astype(F32)
            src[...] = total.astype(BF16)

    def lhs(first, second):
        parts = [
            cp[pl.ds(pl.multiple_of(b * ROWS + core * CORE_ROWS, CORE_ROWS), CORE_ROWS), :]
            for core in (1 - c, c) for b in (first, second)
        ]
        return jnp.concatenate(parts, axis=0)

    def store(v, row, col, where, k):
        for p, ref in enumerate((gv, ow)):
            at = pl.ds(pl.multiple_of(where * CORE_ROWS, CORE_ROWS), CORE_ROWS)
            r = p * 384 + row * CORE_ROWS
            ref[at, k * PIECE : (k + 1) * PIECE] = v[r : r + CORE_ROWS, col * PIECE : (col + 1) * PIECE].astype(BF16)

    def k0(r, k):
        to = (x + r) % 4

        @pl.loop(0, 2)
        def _(n):
            with jax.named_scope("k0"):
                first = (to % 2) * 4 + 2 * n
                v = dot(lhs(first, first + 1), dt[:, pl.ds(pl.multiple_of((to // 2) * 512, 512), 512)])
                for b in range(2):
                    for zz in range(4):
                        store(v, b, zz, (2 * n + b) * 4 + zz, k)

    def k2(t, k):
        @pl.loop(0, 4)
        def _(n):
            with jax.named_scope("k2"):
                v = dot(lhs(2 * n, 2 * n + 1), dt[:, pl.ds(pl.multiple_of(t * 1024 + z * 256, 256), 256)])
                for b in range(2):
                    for hh in range(2):
                        xx, yy = hh * 2 + n // 2, n % 2 * 2 + b
                        store(v, b, hh, yy * 4 + xx, k)

    ups, downs = (x_up, y_up, z_up), (x_dn, y_dn, z_dn)
    place = (x, y, z)
    steps = [(2, 0), (1, 0), (3, 0), (0, 0), (0, 1), (0, 2)]
    index = {s: i for i, s in enumerate(steps)}

    def part(ref, i, start, size):
        return ref.at[pl.ds(start, size), i * PIECE : (i + 1) * PIECE]

    crossed, arrive, held, free = {}, {}, {}, [None] * 4

    def take():
        k = take.next
        take.next = (k + 1) % 4
        if free[k] is not None:
            sent[free[k]].wait_send()
            waited.add(free[k])
        return k

    take.next, waited = 0, set()

    def give(r, t):
        k, i = take(), index[r, t]
        if t:
            k2(t, k)
        else:
            k0(r, k)
        held[i], free[k] = k, len(sent)
        crossed[i] = send(part(gv, k, 0, NBF), part(dr, i, 0, NBF), partner, part(dr, i, 0, NBF))

    def keep(r, t):
        i = index[r, t]
        crossed[i]()
        k = held[i]

        @pl.loop(0, 4)
        def _(b):
            rows = pl.ds(pl.multiple_of(b * 768, 768), 768)
            at = (rows, slice(i * PIECE, (i + 1) * PIECE))
            dr[at] = (ow[rows, k * PIECE : (k + 1) * PIECE].astype(F32) + dr[at].astype(F32)).astype(BF16)

        if r == 2:
            for h, to in ((0, x_up), (1, x_dn)):
                lands = part(rin1, 0, h * HALF, HALF)
                arrive["in", h] = send(part(dr, i, h * HALF, HALF), lands, to, lands)
        elif r:
            side, h, to = (0, 1, x_up) if r == 1 else (1, 0, x_dn)
            lands = part(rf1, side, h * HALF, HALF)
            arrive[side, h] = send(part(dr, i, h * HALF, HALF), lands, to, lands)

    def pass_on(side):
        r, h, to = ((1, 0, x_up), (3, 1, x_dn))[side]
        i = index[r, 0]
        arrive["in", h]()

        @pl.loop(0, 2)
        def _(b):
            rows = pl.ds(pl.multiple_of(h * HALF + b * 768, 768), 768)
            at = (rows, slice(i * PIECE, (i + 1) * PIECE))
            dr[at] = (dr[at].astype(F32) + rin1[rows, :].astype(F32)).astype(BF16)

        lands = part(rf1, side, h * HALF, HALF)
        arrive[side, h] = send(part(dr, i, h * HALF, HALF), lands, to, lands)

    u2(1, z + 2, 1)
    u_begin(1)
    u2(1, z + 1, 2)
    u_direct(1)
    u0(1 - xh)
    give(2, 0)
    u_pass(1)
    u2(2, z + 2, 1)
    u_begin(2)
    keep(2, 0)
    u2(2, z + 1, 2)
    u_direct(2)
    u0(xh)
    give(1, 0)
    give(3, 0)
    keep(1, 0)
    u2(1, z, 1)
    keep(3, 0)
    pass_on(0)
    pass_on(1)
    u_end(1)
    give(0, 1)
    u_pass(2)
    u2(2, z, 1)
    give(0, 0)

    second, third = (1, 1, 1), (2, 0, 0)
    base2 = [place[second[t]] * 768 for t in range(3)]
    levels = ((second, 768, rin2, rf2, (0, 0, 0)), (third, 192, rin3, rf3, base2))
    got = {}

    def summed(level, t, offset, size):
        i = index[0, t]
        row = offset if level == 0 else pl.multiple_of(base2[t] + offset, 32)
        total = dr[pl.ds(row, size), i * PIECE : (i + 1) * PIECE].astype(F32)
        if t == 0:
            for k in range(2):
                total += rf1[pl.ds(row, size), k * PIECE : (k + 1) * PIECE].astype(F32)
        for k in (t, 3 + t):
            if level:
                total += rf2[pl.ds(offset, size), k * PIECE : (k + 1) * PIECE].astype(F32)
        return total

    def put(level, t, offset, v):
        i, base = index[0, t], levels[level][4]
        row = pl.multiple_of(base[t] + offset, 32)
        dr[pl.ds(row, v.shape[0]), i * PIECE : (i + 1) * PIECE] = v.astype(BF16)
        return part(dr, i, row, v.shape[0])

    def begin(level, t):
        axes, size, rin, rf, _ = levels[level]
        half, me = size // 2, place[axes[t]]
        to = ups[axes[t]], downs[axes[t]]
        far = (me + 2) % 4 * size
        for h in range(2):
            at = pl.multiple_of(far + h * half, 32)
            src = put(level, t, at, summed(level, t, at, half))
            lands = part(rin, t, h * half, half)
            got[level, "in", h, t] = send(src, lands, to[h], lands)
        for side, near in ((0, up(me)), (1, down(me))):
            h = 1 - side
            at = pl.multiple_of(near * size + h * half, 32)
            src = put(level, t, at, summed(level, t, at, half))
            lands = part(rf, side * 3 + t, h * half, half)
            got[level, side, h, t] = send(src, lands, to[side], lands)

    def middle(level, t):
        axes, size, rin, rf, _ = levels[level]
        half, me = size // 2, place[axes[t]]
        to = ups[axes[t]], downs[axes[t]]
        for side, near in ((0, up(me)), (1, down(me))):
            h = side
            at = pl.multiple_of(near * size + h * half, 32)
            v = summed(level, t, at, half)
            got[level, "in", h, t]()
            v += rin[h * half : (h + 1) * half, t * PIECE : (t + 1) * PIECE].astype(F32)
            lands = part(rf, side * 3 + t, h * half, half)
            got[level, side, h, t] = send(put(level, t, at, v), lands, to[side], lands)

    def end(level, t):
        for side in range(2):
            for h in range(2):
                got[level, side, h, t]()

    keep(0, 1)
    begin(0, 1)
    keep(0, 0)
    u_end(2)
    give(0, 2)
    middle(0, 1)
    for side in range(2):
        for h in range(2):
            arrive[side, h]()
    begin(0, 0)
    keep(0, 2)
    begin(0, 2)
    end(0, 1)
    begin(1, 1)
    middle(0, 0)
    middle(0, 2)
    middle(1, 1)
    end(0, 0)
    begin(1, 0)
    end(0, 2)
    begin(1, 2)
    middle(1, 0)
    middle(1, 2)
    for t in (1, 0, 2):
        end(1, t)
        total = summed(1, t, pl.multiple_of(place[third[t]] * CORE_ROWS, 32), CORE_ROWS)
        for k in (t, 3 + t):
            total += rf3[:, k * PIECE : (k + 1) * PIECE].astype(F32)
        out_ref[:, t * PIECE : (t + 1) * PIECE] = total

    for i in range(gathered, len(sent)):
        if i not in waited:
            sent[i].wait_send()


def local(collocation, density, kernel_values):
    coefficients = kernel_values.reshape(PANEL * 16, PIECE)
    return pl.pallas_call(
        kernel,
        out_shape=jax.ShapeDtypeStruct((CORE_ROWS, ROWS), F32),
        in_specs=[pl.BlockSpec(memory_space=pl.ANY)] * 3,
        out_specs=pl.BlockSpec(memory_space=pltpu.VMEM),
        scratch_shapes=[
            pltpu.VMEM((NBF, PANEL), BF16),
            pltpu.VMEM((ROWS, NBF), BF16),
            pltpu.VMEM((PANEL, NBF), BF16),
            pltpu.VMEM((NBF, NQ), BF16),
            pltpu.VMEM((PANEL, NQ), BF16),
            pltpu.VMEM((PANEL, NQ), F32),
            pltpu.VMEM((1024, PIECE), F32),
            pltpu.VMEM((4, 256, ROWS), BF16),
            pltpu.VMEM((NBF, 4 * PIECE), BF16),
            pltpu.VMEM((NBF, 4 * PIECE), BF16),
            pltpu.VMEM((NBF, 6 * PIECE), BF16),
            pltpu.VMEM((PANEL, 2 * 256), BF16),
            pltpu.VMEM((PANEL, 4 * 256), BF16),
            pltpu.VMEM((NBF, PIECE), BF16),
            pltpu.VMEM((NBF, 2 * PIECE), BF16),
            pltpu.VMEM((768, 3 * PIECE), BF16),
            pltpu.VMEM((768, 6 * PIECE), BF16),
            pltpu.VMEM((192, 3 * PIECE), BF16),
            pltpu.VMEM((192, 6 * PIECE), BF16),
            pltpu.SemaphoreType.DMA((N_SENDS,)),
            pltpu.SemaphoreType.DMA((N_SENDS,)),
            pltpu.SemaphoreType.DMA((12,)),
        ],
        compiler_params=pltpu.CompilerParams(
            collective_id=0, has_side_effects=True, vmem_limit_bytes=67043328
        ),
    )(collocation, density, coefficients)


def solution(mesh):
    return jax.shard_map(
        local,
        mesh=mesh,
        in_specs=(P(None, "gx"), P("gy", None), P("gx", None, "gy", None)),
        out_specs=P("gx", "gy"),
        check_vma=False,
    )
```

```python
import jax
import jax.numpy as jnp
from jax import lax
from jax.experimental import pallas as pl
from jax.experimental.pallas import tpu as pltpu
from jax.sharding import PartitionSpec as P

MESH = pl.DeviceIdType.MESH
BF16 = jnp.bfloat16
F32 = jnp.float32

NBF = 3072
PANEL = 1024
PIECE = 128
ROWS = 384
NQ = 2048
HALF = NBF // 2
CORE_ROWS = 192
N_SENDS = 160


def dot(a, b):
    return jnp.dot(a, b, preferred_element_type=F32)


def kernel(
    c_ref, d_ref, z_ref, out_ref,
    cp, dv, dt, cq, zw, acc, zf, rel, relb, gv, ow, dr, uin, uf, rin1, rf1, rin2, rf2, rin3, rf3,
    send_sem, recv_sem, local_sem,
):
    gx, gy = lax.axis_index("gx"), lax.axis_index("gy")
    c, y, xl = gx % 2, (gx // 2) % 4, gx // 8
    z, xh = gy // 2, gy % 2
    x = xh * 2 + xl
    once = 1 + gx // 16

    def device(x, y, z, c):
        return {"gx": ((x % 2) * 4 + y) * 2 + c, "gy": z * 2 + x // 2}

    def up(v):
        return (v + 1) % 4

    def down(v):
        return (v + 3) % 4

    partner = device(x, y, z, 1 - c)
    x_up, x_dn = device(up(x), y, z, c), device(down(x), y, z, c)
    y_up, y_dn = device(x, up(y), z, c), device(x, down(y), z, c)
    z_up, z_dn = device(x, y, up(z), c), device(x, y, down(z), c)

    barrier = pltpu.get_barrier_semaphore()
    neighbours = (partner, x_up, x_dn, y_up, y_dn, z_up, z_dn)
    for one in neighbours:
        pl.semaphore_signal(barrier, inc=1, device_id=one, device_id_type=MESH)

    locals_ = []

    def fetch(src, dst):
        copy = pltpu.make_async_copy(src, dst, local_sem.at[len(locals_)])
        copy.start()
        locals_.append(copy)
        return copy

    def column(ref, k, rows=None, width=PIECE):
        cols = pl.ds(pl.multiple_of(k * width, PIECE), width)
        return ref.at[:, cols] if rows is None else ref.at[pl.ds(*rows), cols]

    d_in = fetch(d_ref, dv)
    cp_in = [fetch(column(c_ref, i, width=256), column(cp, i, width=256)) for i in range(4)]
    own_in = fetch(column(c_ref, gy), column(cq, gx))
    sent = []

    def send(src, dst, to, lands):
        i = len(sent)
        copy = pltpu.make_async_remote_copy(
            src_ref=src, dst_ref=dst, send_sem=send_sem.at[i], recv_sem=recv_sem.at[i],
            device_id=to, device_id_type=MESH,
        )
        copy.start()
        sent.append(copy)
        arrival = pltpu.make_async_remote_copy(
            src_ref=lands, dst_ref=lands, send_sem=send_sem.at[i], recv_sem=recv_sem.at[i],
            device_id=to, device_id_type=MESH,
        )
        return arrival.wait_recv

    def slot(xl, y, c):
        return (xl * 4 + y) * 2 + c

    low, high = (0, HALF), (HALF, HALF)

    def piece(k, rows=None):
        return column(cq, k, rows)

    def relay_piece(k, to, mine, rows=None):
        return send(piece(k, rows), piece(k, rows), to, piece(mine, rows))

    own_cols = pl.ds(pl.multiple_of(gy * ROWS, PIECE), ROWS)

    def dense(q):
        cp_in[q].wait()

        @pl.loop(0, once)
        def _(_i):
            with jax.named_scope(f"own{q}"):
                rows = dot(dv[...], cp[:, q * 256 : (q + 1) * 256])
                dt[q * 256 : (q + 1) * 256, own_cols] = rows.T.astype(BF16)

    d_in.wait()
    dense(0)
    pl.semaphore_wait(barrier, len(neighbours))

    own_in.wait()
    own = piece(gx)
    y_own_dn = send(own, piece(gx), y_up, piece(slot(xl, down(y), c)))
    y_own_up = send(own, piece(gx), y_dn, piece(slot(xl, up(y), c)))
    other = slot(1 - xl, y, c)
    x_lo = send(column(c_ref, z * 2 + up(x) // 2, low), piece(gx, low), x_up, piece(other, low))
    x_hi = send(column(c_ref, z * 2 + down(x) // 2, high), piece(gx, high), x_dn, piece(other, high))
    near = [send(own, piece(gx), partner, piece(slot(xl, y, 1 - c)))]

    def block(j, q):
        return dt.at[pl.ds(q * 256, 256), pl.ds(pl.multiple_of(j * ROWS, PIECE), ROWS)]

    def group(x, z):
        return z * 2 + x // 2

    def both(j, q, xz):
        return (
            send(block(j, q), block(j, q), z_up, block(group(xz, down(z)), q)),
            send(block(j, q), block(j, q), z_dn, block(group(xz, up(z)), q)),
        )

    def onward(q, xz):
        b = block(group(xz, (down(z), up(z))[q % 2]), q)
        return send(b, b, (z_up, z_dn)[q % 2], block(group(xz, (z + 2) % 4), q))

    z_own, relayed = [], []
    for q in range(4):
        if q:
            dense(q)
        z_own.append(both(gy, q, x))
        if q < 3:
            relayed.append(send(block(gy, q), rel.at[q], (x_up, x_dn)[q % 2], rel.at[q]))

    z_in = []
    for i in range(6):
        ref, rows = (gv, ow)[i // 4], min(NBF, PANEL * 16 - i * NBF)
        z_in.append(fetch(z_ref.at[pl.ds(i * NBF, rows)], column(ref, i % 4, (0, rows))))

    def unpack(i):
        ref, n = (gv, ow)[i // 4], min(CORE_ROWS, PANEL - i * CORE_ROWS)
        z_in[i].wait()

        @pl.loop(0, n // 64)
        def _(b):
            with jax.named_scope("unpack"):
                first = pl.multiple_of(b * 1024, 1024)
                zf[...] = ref[pl.ds(first, 1024), (i % 4) * PIECE : (i % 4 + 1) * PIECE].astype(F32)
                to = pl.ds(pl.multiple_of(i * CORE_ROWS + b * 64, 64), 64)
                for k in range(16):
                    zw[to, k * PIECE : (k + 1) * PIECE] = zf[pl.ds(k, 64, stride=16), :].astype(BF16)

    x_far, z_far, next_own, next_far = {}, {}, {}, {}
    far = (x + 2) % 4

    def forward(q):
        relayed[q]()
        origin = group((down(x), up(x))[q % 2], z)
        x_far[q] = send(rel.at[q], block(origin, q), (x_up, x_dn)[q % 2], block(group(far, z), q))

    four = (z, down(z), up(z), (z + 2) % 4)
    crossing, landing = {}, []

    def half(j, h):
        return dt.at[pl.ds(768 + h * 128, 128), pl.ds(pl.multiple_of(j * ROWS, PIECE), ROWS)]

    def cross(i):
        for h, to in ((0, x_up), (1, x_dn)):
            lands = relb.at[i, pl.ds(h * 128, 128), :]
            crossing[i, h] = send(half(group(x, four[i]), h), lands, to, lands)

    def land(i):
        for h, origin, to in ((0, down(x), x_up), (1, up(x), x_dn)):
            crossing[i, h]()
            src = relb.at[i, pl.ds(h * 128, 128), :]
            landing.append(send(src, half(group(origin, four[i]), h), to, half(group(far, four[i]), h)))

    unpack(0)
    unpack(1)
    y_other = []
    for wait, rows in ((x_lo, low), (x_hi, high)):
        wait()
        k = other
        y_other.append((
            relay_piece(k, y_up, slot(1 - xl, down(y), c), rows),
            relay_piece(k, y_dn, slot(1 - xl, up(y), c), rows),
        ))
        near.append(relay_piece(k, partner, slot(1 - xl, y, 1 - c), rows))
    z_own[0][0]()
    next_own[0] = onward(0, x)
    z_own[1][1]()
    next_own[1] = onward(1, x)
    forward(0)
    forward(1)
    y_own_dn()
    far_lo = relay_piece(slot(xl, down(y), c), y_up, slot(xl, (y + 2) % 4, c), low)
    near.append(relay_piece(slot(xl, down(y), c), partner, slot(xl, down(y), 1 - c)))
    y_own_up()
    far_hi = relay_piece(slot(xl, up(y), c), y_dn, slot(xl, (y + 2) % 4, c), high)
    near.append(relay_piece(slot(xl, up(y), c), partner, slot(xl, up(y), 1 - c)))
    z_own[2][0]()
    next_own[2] = onward(2, x)
    forward(2)
    z_own[3][1]()
    next_own[3] = onward(3, x)
    cross(0)
    cross(2)
    unpack(2)
    for q in range(3):
        x_far[q]()
        z_far[q] = both(group(far, z), q, far)
        unpack(3 + q)
    z_own[3][0]()
    cross(1)
    land(0)

    def wpart(which, s):
        cols = pl.ds(pl.multiple_of(s * 256, 256), 256)
        near_js = [2 * zz + xh for zz in range(4)]
        far_js = [2 * ((z + i) % 4) + 1 - xh for i in (0, 1, 3)]
        last_js = [2 * ((z + 2) % 4) + 1 - xh]
        js = {"near": near_js, "far": far_js, "last": last_js, "all": near_js + far_js + last_js}[which]
        with jax.named_scope("m" + which):
            at = [pl.ds(pl.multiple_of(j * ROWS, PIECE), ROWS) for j in js]
            if which == "all":
                v = dot(dt[...], cq[:, cols])
            else:
                v = dot(jnp.concatenate([dt[:, a] for a in at], axis=1), jnp.concatenate([cq[a, cols] for a in at], axis=0))
            if which == "near":
                acc[:, cols] = v
            elif which == "far":
                acc[:, cols] += v
            else:
                v = v if which == "all" else v + acc[:, cols]
                zw[:, cols] = (zw[:, cols].astype(F32) * v).astype(BF16)

    for wait in near:
        wait()
    for wait in (z_own[0][1], z_own[1][0], z_own[2][1], next_own[0], next_own[1], next_own[2], next_own[3]):
        wait()
    cross(3)
    land(2)

    @pl.loop(0, 4)
    def _(i):
        wpart("near", jnp.where(i == 3, (1 - xl) * 4 + y, xl * 4 + (y + i + i // 2) % 4))

    passed = []
    k = slot(1 - xl, down(y), c)
    y_other[0][0]()
    far_other_lo = relay_piece(k, y_up, slot(1 - xl, (y + 2) % 4, c), low)
    passed.append(relay_piece(k, partner, slot(1 - xl, down(y), 1 - c), low))
    k = slot(1 - xl, up(y), c)
    y_other[1][1]()
    far_other_hi = relay_piece(k, y_dn, slot(1 - xl, (y + 2) % 4, c), high)
    passed.append(relay_piece(k, partner, slot(1 - xl, up(y), 1 - c), high))
    z_far[0][0]()
    next_far[0] = onward(0, far)
    y_other[1][0]()
    k = slot(1 - xl, down(y), c)
    passed.append(relay_piece(k, partner, slot(1 - xl, down(y), 1 - c), high))
    y_other[0][1]()
    k = slot(1 - xl, up(y), c)
    passed.append(relay_piece(k, partner, slot(1 - xl, up(y), 1 - c), low))
    z_far[1][1]()
    next_far[1] = onward(1, far)
    for wait in passed:
        wait()

    @pl.loop(0, 2)
    def _(i):
        wpart("near", (1 - xl) * 4 + (y + 1 + 2 * i) % 4)

    land(1)
    z_far[2][0]()
    next_far[2] = onward(2, far)
    land(3)
    passed = []
    for wait, rows in ((far_lo, low), (far_hi, high)):
        wait()
        k = slot(xl, (y + 2) % 4, c)
        passed.append(relay_piece(k, partner, slot(xl, (y + 2) % 4, 1 - c), rows))
    for wait in passed:
        wait()

    @pl.loop(0, once)
    def _(_i):
        wpart("near", xl * 4 + (y + 2) % 4)

    for wait in (z_far[0][1], z_far[1][0], z_far[2][1], *landing[:6]):
        wait()
    newest = (1 - xl) * 4 + (y + 2) % 4

    @pl.loop(0, 7)
    def _(i):
        wpart("far", (newest + 1 + i) % 8)

    passed = []
    for wait, rows in ((far_other_lo, low), (far_other_hi, high)):
        wait()
        k = slot(1 - xl, (y + 2) % 4, c)
        passed.append(relay_piece(k, partner, slot(1 - xl, (y + 2) % 4, 1 - c), rows))
    for q in range(3):
        next_far[q]()
    for wait in landing[6:]:
        wait()

    @pl.loop(0, 7)
    def _(i):
        wpart("last", (newest + 1 + i) % 8)

    for wait in passed:
        wait()

    @pl.loop(0, once)
    def _(_i):
        wpart("all", newest)

    for copy in sent:
        copy.wait_send()
    gathered = len(sent)

    def u(t, first, second, col):
        rows = [cq[pl.ds(pl.multiple_of(g * ROWS + t * PIECE, PIECE), PIECE), :] for g in (first, second)]
        with jax.named_scope("u"):
            v = lax.dot_general(
                zw[...], jnp.concatenate(rows, axis=0), (((1,), (1,)), ((), ())), preferred_element_type=F32
            )
            dt[:, pl.ds(pl.multiple_of(col, 256), 256)] = v.astype(BF16)

    def u0(xh):
        @pl.loop(0, 2)
        def _(p):
            u(0, 4 * p + xh, 4 * p + 2 + xh, xh * 512 + p * 256)

    def u2(t, first, count):
        @pl.loop(0, count * once)
        def _(p):
            zz = (first + 2 * p) % 4
            u(t, 2 * zz, 2 * zz + 1, t * 1024 + zz * 256)

    def upart(t, r, h):
        return dt.at[pl.ds(h * 512, 512), pl.ds(pl.multiple_of(t * 1024 + (z + r) % 4 * 256, 256), 256)]

    def uplace(ref, i, h):
        return ref.at[pl.ds(h * 512, 512), i * 256 : (i + 1) * 256]

    moved = {}

    def u_begin(t):
        for h, to in ((0, z_up), (1, z_dn)):
            lands = uplace(uin, t - 1, h)
            moved["in", h, t] = send(upart(t, 2, h), lands, to, lands)

    def u_direct(t):
        for side, r, h, to in ((0, 1, 1, z_up), (1, 3, 0, z_dn)):
            lands = uplace(uf, 2 * side + t - 1, h)
            moved[side, h, t] = send(upart(t, r, h), lands, to, lands)

    def u_pass(t):
        for side, r, h, to in ((0, 1, 0, z_up), (1, 3, 1, z_dn)):
            moved["in", h, t]()
            src = upart(t, r, h)
            src[...] = (src[...].astype(F32) + uplace(uin, t - 1, h)[...].astype(F32)).astype(BF16)
            lands = uplace(uf, 2 * side + t - 1, h)
            moved[side, h, t] = send(src, lands, to, lands)

    def u_end(t):
        for h in range(2):
            moved[0, h, t]()
            moved[1, h, t]()
            src = upart(t, 0, h)
            total = src[...].astype(F32)
            for side in range(2):
                total += uplace(uf, 2 * side + t - 1, h)[...].astype(F32)
            src[...] = total.astype(BF16)

    def lhs(first, second):
        parts = [
            cp[pl.ds(pl.multiple_of(b * ROWS + core * CORE_ROWS, CORE_ROWS), CORE_ROWS), :]
            for core in (1 - c, c) for b in (first, second)
        ]
        return jnp.concatenate(parts, axis=0)

    def store(v, row, col, where, k):
        for p, ref in enumerate((gv, ow)):
            at = pl.ds(pl.multiple_of(where * CORE_ROWS, CORE_ROWS), CORE_ROWS)
            r = p * 384 + row * CORE_ROWS
            ref[at, k * PIECE : (k + 1) * PIECE] = v[r : r + CORE_ROWS, col * PIECE : (col + 1) * PIECE].astype(BF16)

    def k0(r, k):
        to = (x + r) % 4

        @pl.loop(0, 2)
        def _(n):
            with jax.named_scope("k0"):
                first = (to % 2) * 4 + 2 * n
                v = dot(lhs(first, first + 1), dt[:, pl.ds(pl.multiple_of((to // 2) * 512, 512), 512)])
                for b in range(2):
                    for zz in range(4):
                        store(v, b, zz, zz * 4 + 2 * n + b, k)

    def k2(t, k, core, ref):
        @pl.loop(0, 2)
        def _(n):
            with jax.named_scope("k2"):
                rows = [cp[pl.ds(pl.multiple_of((4 * n + b) * ROWS + core * CORE_ROWS, CORE_ROWS), CORE_ROWS), :] for b in range(4)]
                v = dot(jnp.concatenate(rows, axis=0), dt[:, pl.ds(pl.multiple_of(t * 1024 + z * 256, 256), 256)])
                for b in range(4):
                    for hh in range(2):
                        at = pl.ds(pl.multiple_of((b * 4 + hh * 2 + n) * CORE_ROWS, CORE_ROWS), CORE_ROWS)
                        block = v[b * CORE_ROWS : (b + 1) * CORE_ROWS, hh * PIECE : (hh + 1) * PIECE]
                        ref[at, k * PIECE : (k + 1) * PIECE] = block.astype(BF16)

    ups, downs = (x_up, y_up, z_up), (x_dn, y_dn, z_dn)
    place = (x, y, z)
    steps = [(2, 0), (1, 0), (3, 0), (0, 0), (0, 1), (0, 2)]
    index = {s: i for i, s in enumerate(steps)}

    def part(ref, i, start, size):
        return ref.at[pl.ds(start, size), i * PIECE : (i + 1) * PIECE]

    crossed, arrive, held, free = {}, {}, {}, [None] * 4

    def take():
        k = take.next
        take.next = (k + 1) % 4
        if free[k] is not None:
            sent[free[k]].wait_send()
            waited.add(free[k])
        return k

    take.next, waited = 0, set()

    def give(r, t):
        k, i = take(), index[r, t]
        if t:
            k2(t, k, 1 - c, gv)
        else:
            k0(r, k)
        held[i], free[k] = k, len(sent)
        crossed[i] = send(part(gv, k, 0, NBF), part(dr, i, 0, NBF), partner, part(dr, i, 0, NBF))
        if t:
            k2(t, k, c, ow)

    def keep(r, t):
        i = index[r, t]
        crossed[i]()
        k = held[i]

        @pl.loop(0, 4)
        def _(b):
            rows = pl.ds(pl.multiple_of(b * 768, 768), 768)
            at = (rows, slice(i * PIECE, (i + 1) * PIECE))
            dr[at] = (ow[rows, k * PIECE : (k + 1) * PIECE].astype(F32) + dr[at].astype(F32)).astype(BF16)

        if r == 2:
            for h, to in ((0, x_up), (1, x_dn)):
                lands = part(rin1, 0, h * HALF, HALF)
                arrive["in", h] = send(part(dr, i, h * HALF, HALF), lands, to, lands)
        elif r:
            side, h, to = (0, 1, x_up) if r == 1 else (1, 0, x_dn)
            lands = part(rf1, side, h * HALF, HALF)
            arrive[side, h] = send(part(dr, i, h * HALF, HALF), lands, to, lands)

    def pass_on(side):
        r, h, to = ((1, 0, x_up), (3, 1, x_dn))[side]
        i = index[r, 0]
        arrive["in", h]()

        @pl.loop(0, 2)
        def _(b):
            rows = pl.ds(pl.multiple_of(h * HALF + b * 768, 768), 768)
            at = (rows, slice(i * PIECE, (i + 1) * PIECE))
            dr[at] = (dr[at].astype(F32) + rin1[rows, :].astype(F32)).astype(BF16)

        lands = part(rf1, side, h * HALF, HALF)
        arrive[side, h] = send(part(dr, i, h * HALF, HALF), lands, to, lands)

    u2(1, z + 2, 1)
    u_begin(1)
    u0(1 - xh)
    give(2, 0)
    u2(2, z + 2, 1)
    u_begin(2)
    u2(1, z + 1, 2)
    u_direct(1)
    keep(2, 0)
    u0(xh)
    u_pass(1)
    give(1, 0)
    give(3, 0)
    keep(1, 0)
    u2(2, z + 1, 1)
    keep(3, 0)
    u2(2, z + 3, 1)
    u_direct(2)
    pass_on(0)
    pass_on(1)
    u_pass(2)
    u2(1, z, 1)
    u2(2, z, 1)
    give(0, 0)
    u_end(1)
    give(0, 1)
    keep(0, 0)

    second, third = (2, 1, 1), (1, 0, 0)
    base2 = [place[second[t]] * 768 for t in range(3)]
    levels = ((second, 768, rin2, rf2, (0, 0, 0)), (third, 192, rin3, rf3, base2))
    got = {}

    def summed(level, t, offset, size):
        i = index[0, t]
        row = offset if level == 0 else pl.multiple_of(base2[t] + offset, 32)
        total = dr[pl.ds(row, size), i * PIECE : (i + 1) * PIECE].astype(F32)
        if t == 0:
            for k in range(2):
                total += rf1[pl.ds(row, size), k * PIECE : (k + 1) * PIECE].astype(F32)
        for k in (t, 3 + t):
            if level:
                total += rf2[pl.ds(offset, size), k * PIECE : (k + 1) * PIECE].astype(F32)
        return total

    def put(level, t, offset, v):
        i, base = index[0, t], levels[level][4]
        row = pl.multiple_of(base[t] + offset, 32)
        dr[pl.ds(row, v.shape[0]), i * PIECE : (i + 1) * PIECE] = v.astype(BF16)
        return part(dr, i, row, v.shape[0])

    def begin(level, t, which=(2, 0, 1)):
        axes, size, rin, rf, _ = levels[level]
        half, me = size // 2, place[axes[t]]
        to = ups[axes[t]], downs[axes[t]]
        far = (me + 2) % 4 * size
        for h in range(2) if 2 in which else ():
            at = pl.multiple_of(far + h * half, 32)
            src = put(level, t, at, summed(level, t, at, half))
            lands = part(rin, t, h * half, half)
            got[level, "in", h, t] = send(src, lands, to[h], lands)
        for side, near in ((0, up(me)), (1, down(me))):
            if side not in which:
                continue
            h = 1 - side
            at = pl.multiple_of(near * size + h * half, 32)
            src = put(level, t, at, summed(level, t, at, half))
            lands = part(rf, side * 3 + t, h * half, half)
            got[level, side, h, t] = send(src, lands, to[side], lands)

    def middle(level, t):
        axes, size, rin, rf, _ = levels[level]
        half, me = size // 2, place[axes[t]]
        to = ups[axes[t]], downs[axes[t]]
        for side, near in ((0, up(me)), (1, down(me))):
            h = side
            at = pl.multiple_of(near * size + h * half, 32)
            v = summed(level, t, at, half)
            got[level, "in", h, t]()
            v += rin[h * half : (h + 1) * half, t * PIECE : (t + 1) * PIECE].astype(F32)
            lands = part(rf, side * 3 + t, h * half, half)
            got[level, side, h, t] = send(put(level, t, at, v), lands, to[side], lands)

    def end(level, t):
        for side in range(2):
            for h in range(2):
                got[level, side, h, t]()

    def finish(t):
        end(1, t)
        total = summed(1, t, pl.multiple_of(place[third[t]] * CORE_ROWS, 32), CORE_ROWS)
        for k in (t, 3 + t):
            total += rf3[:, k * PIECE : (k + 1) * PIECE].astype(F32)
        out_ref[:, t * PIECE : (t + 1) * PIECE] = total

    k_last = take()
    i_last = index[0, 2]
    over = {}

    def give_y(dy):
        yy = (y + dy) % 4

        @pl.loop(0, once)
        def _(_i):
            with jax.named_scope("ky"):
                v = dot(lhs(yy, 4 + yy), dt[:, pl.ds(pl.multiple_of(2048 + z * 256, 256), 256)])
                for b in range(2):
                    for hh in range(2):
                        store(v, b, hh, yy * 4 + hh * 2 + b, k_last)

        rows = pl.multiple_of(yy * 768, 768)
        over[dy] = send(part(gv, k_last, rows, 768), part(dr, i_last, rows, 768), partner, part(dr, i_last, rows, 768))

    def keep_y(dy):
        over[dy]()
        rows = pl.ds(pl.multiple_of((y + dy) % 4 * 768, 768), 768)
        at = (rows, slice(i_last * PIECE, (i_last + 1) * PIECE))
        dr[at] = (ow[rows, k_last * PIECE : (k_last + 1) * PIECE].astype(F32) + dr[at].astype(F32)).astype(BF16)

    keep(0, 1)
    begin(0, 1)
    for side in range(2):
        for h in range(2):
            arrive[side, h]()
    begin(0, 0)
    middle(0, 1)
    u_end(2)
    give_y(2)
    give_y(1)
    keep_y(2)
    begin(0, 2, (2,))
    give_y(3)
    keep_y(1)
    begin(0, 2, (0,))
    give_y(0)
    keep_y(3)
    begin(0, 2, (1,))
    end(0, 1)
    begin(1, 1)
    keep_y(0)
    middle(0, 0)
    middle(0, 2)
    end(0, 0)
    begin(1, 0)
    middle(1, 1)
    end(0, 2)
    begin(1, 2)
    middle(1, 0)
    finish(1)
    middle(1, 2)
    finish(0)
    finish(2)

    for i in range(gathered, len(sent)):
        if i not in waited:
            sent[i].wait_send()


def local(collocation, density, kernel_values):
    coefficients = kernel_values.reshape(PANEL * 16, PIECE)
    return pl.pallas_call(
        kernel,
        out_shape=jax.ShapeDtypeStruct((CORE_ROWS, ROWS), F32),
        in_specs=[pl.BlockSpec(memory_space=pl.ANY)] * 3,
        out_specs=pl.BlockSpec(memory_space=pltpu.VMEM),
        scratch_shapes=[
            pltpu.VMEM((NBF, PANEL), BF16),
            pltpu.VMEM((ROWS, NBF), BF16),
            pltpu.VMEM((PANEL, NBF), BF16),
            pltpu.VMEM((NBF, NQ), BF16),
            pltpu.VMEM((PANEL, NQ), BF16),
            pltpu.VMEM((PANEL, NQ), F32),
            pltpu.VMEM((1024, PIECE), F32),
            pltpu.VMEM((3, 256, ROWS), BF16),
            pltpu.VMEM((4, 256, ROWS), BF16),
            pltpu.VMEM((NBF, 4 * PIECE), BF16),
            pltpu.VMEM((NBF, 4 * PIECE), BF16),
            pltpu.VMEM((NBF, 6 * PIECE), BF16),
            pltpu.VMEM((PANEL, 2 * 256), BF16),
            pltpu.VMEM((PANEL, 4 * 256), BF16),
            pltpu.VMEM((NBF, PIECE), BF16),
            pltpu.VMEM((NBF, 2 * PIECE), BF16),
            pltpu.VMEM((768, 3 * PIECE), BF16),
            pltpu.VMEM((768, 6 * PIECE), BF16),
            pltpu.VMEM((192, 3 * PIECE), BF16),
            pltpu.VMEM((192, 6 * PIECE), BF16),
            pltpu.SemaphoreType.DMA((N_SENDS,)),
            pltpu.SemaphoreType.DMA((N_SENDS,)),
            pltpu.SemaphoreType.DMA((12,)),
        ],
        compiler_params=pltpu.CompilerParams(
            collective_id=0, has_side_effects=True, vmem_limit_bytes=67043328
        ),
    )(collocation, density, coefficients)


def solution(mesh):
    return jax.shard_map(
        local,
        mesh=mesh,
        in_specs=(P(None, "gx"), P("gy", None), P("gx", None, "gy", None)),
        out_specs=P("gx", "gy"),
        check_vma=False,
    )
```

```python
import jax
import jax.numpy as jnp
from jax import lax
from jax.experimental import pallas as pl
from jax.experimental.pallas import tpu as pltpu
from jax.sharding import PartitionSpec as P

MESH = pl.DeviceIdType.MESH
BF16 = jnp.bfloat16
F32 = jnp.float32

NBF = 3072
PANEL = 1024
PIECE = 128
ROWS = 384
NQ = 2048
HALF = NBF // 2
CORE_ROWS = 192
N_SENDS = 160


def dot(a, b):
    return jnp.dot(a, b, preferred_element_type=F32)


def kernel(
    c_ref, d_ref, z_ref, out_ref,
    cp, dv, dt, cq, zw, acc, zf, rel, relb, gv, ow, dr, uin, uf, rin1, rf1, rin2, rf2, rf3,
    send_sem, recv_sem, local_sem,
):
    gx, gy = lax.axis_index("gx"), lax.axis_index("gy")
    c, y, xl = gx % 2, (gx // 2) % 4, gx // 8
    z, xh = gy // 2, gy % 2
    x = xh * 2 + xl
    once = 1 + gx // 16

    def device(x, y, z, c):
        return {"gx": ((x % 2) * 4 + y) * 2 + c, "gy": z * 2 + x // 2}

    def up(v):
        return (v + 1) % 4

    def down(v):
        return (v + 3) % 4

    partner = device(x, y, z, 1 - c)
    x_up, x_dn = device(up(x), y, z, c), device(down(x), y, z, c)
    y_up, y_dn = device(x, up(y), z, c), device(x, down(y), z, c)
    z_up, z_dn = device(x, y, up(z), c), device(x, y, down(z), c)

    x_across, y_across = device((x + 2) % 4, y, z, c), device(x, (y + 2) % 4, z, c)

    barrier = pltpu.get_barrier_semaphore()
    neighbours = (x_across, y_across, partner, x_up, x_dn, y_up, y_dn, z_up, z_dn)
    for one in neighbours:
        pl.semaphore_signal(barrier, inc=1, device_id=one, device_id_type=MESH)

    locals_ = []

    def fetch(src, dst):
        copy = pltpu.make_async_copy(src, dst, local_sem.at[len(locals_)])
        copy.start()
        locals_.append(copy)
        return copy

    def column(ref, k, rows=None, width=PIECE):
        cols = pl.ds(pl.multiple_of(k * width, PIECE), width)
        return ref.at[:, cols] if rows is None else ref.at[pl.ds(*rows), cols]

    d_in = fetch(d_ref, dv)
    cp_in = [fetch(column(c_ref, i, width=256), column(cp, i, width=256)) for i in range(4)]
    own_in = fetch(column(c_ref, gy), column(cq, gx))
    sent = []

    def send(src, dst, to, lands):
        i = len(sent)
        copy = pltpu.make_async_remote_copy(
            src_ref=src, dst_ref=dst, send_sem=send_sem.at[i], recv_sem=recv_sem.at[i],
            device_id=to, device_id_type=MESH,
        )
        copy.start()
        sent.append(copy)
        arrival = pltpu.make_async_remote_copy(
            src_ref=lands, dst_ref=lands, send_sem=send_sem.at[i], recv_sem=recv_sem.at[i],
            device_id=to, device_id_type=MESH,
        )
        return arrival.wait_recv

    def slot(xl, y, c):
        return (xl * 4 + y) * 2 + c

    low, high = (0, HALF), (HALF, HALF)

    def piece(k, rows=None):
        return column(cq, k, rows)

    def relay_piece(k, to, mine, rows=None):
        return send(piece(k, rows), piece(k, rows), to, piece(mine, rows))

    own_cols = pl.ds(pl.multiple_of(gy * ROWS, PIECE), ROWS)

    def dense(q):
        cp_in[q].wait()

        @pl.loop(0, once)
        def _(_i):
            with jax.named_scope(f"own{q}"):
                rows = dot(dv[...], cp[:, q * 256 : (q + 1) * 256])
                dt[q * 256 : (q + 1) * 256, own_cols] = rows.T.astype(BF16)

    d_in.wait()
    dense(0)
    pl.semaphore_wait(barrier, len(neighbours))

    own_in.wait()
    own = piece(gx)
    y_own_dn = send(own, piece(gx), y_up, piece(slot(xl, down(y), c)))
    y_own_up = send(own, piece(gx), y_dn, piece(slot(xl, up(y), c)))
    other = slot(1 - xl, y, c)
    x_lo = send(column(c_ref, z * 2 + up(x) // 2, low), piece(gx, low), x_up, piece(other, low))
    x_hi = send(column(c_ref, z * 2 + down(x) // 2, high), piece(gx, high), x_dn, piece(other, high))
    near = [send(own, piece(gx), partner, piece(slot(xl, y, 1 - c)))]

    def block(j, q):
        return dt.at[pl.ds(q * 256, 256), pl.ds(pl.multiple_of(j * ROWS, PIECE), ROWS)]

    def group(x, z):
        return z * 2 + x // 2

    def both(j, q, xz):
        return (
            send(block(j, q), block(j, q), z_up, block(group(xz, down(z)), q)),
            send(block(j, q), block(j, q), z_dn, block(group(xz, up(z)), q)),
        )

    def onward(q, xz):
        b = block(group(xz, (down(z), up(z))[q % 2]), q)
        return send(b, b, (z_up, z_dn)[q % 2], block(group(xz, (z + 2) % 4), q))

    z_own, relayed = [], []
    for q in range(4):
        if q:
            dense(q)
        z_own.append(both(gy, q, x))
        if q < 3:
            relayed.append(send(block(gy, q), rel.at[q], (x_up, x_dn)[q % 2], rel.at[q]))

    z_in = []
    for i in range(6):
        ref, rows = (gv, ow)[i // 4], min(NBF, PANEL * 16 - i * NBF)
        z_in.append(fetch(z_ref.at[pl.ds(i * NBF, rows)], column(ref, i % 4, (0, rows))))

    def unpack(i):
        ref, n = (gv, ow)[i // 4], min(CORE_ROWS, PANEL - i * CORE_ROWS)
        z_in[i].wait()

        @pl.loop(0, n // 64)
        def _(b):
            with jax.named_scope("unpack"):
                first = pl.multiple_of(b * 1024, 1024)
                zf[...] = ref[pl.ds(first, 1024), (i % 4) * PIECE : (i % 4 + 1) * PIECE].astype(F32)
                to = pl.ds(pl.multiple_of(i * CORE_ROWS + b * 64, 64), 64)
                for k in range(16):
                    zw[to, k * PIECE : (k + 1) * PIECE] = zf[pl.ds(k, 64, stride=16), :].astype(BF16)

    x_far, z_far, next_own, next_far = {}, {}, {}, {}
    far = (x + 2) % 4

    def forward(q):
        relayed[q]()
        origin = group((down(x), up(x))[q % 2], z)
        x_far[q] = send(rel.at[q], block(origin, q), (x_up, x_dn)[q % 2], block(group(far, z), q))

    four = (z, down(z), up(z), (z + 2) % 4)
    crossing, landing = {}, []

    def half(j, h):
        return dt.at[pl.ds(768 + h * 128, 128), pl.ds(pl.multiple_of(j * ROWS, PIECE), ROWS)]

    def cross(i):
        for h, to in ((0, x_up), (1, x_dn)):
            lands = relb.at[i, pl.ds(h * 128, 128), :]
            crossing[i, h] = send(half(group(x, four[i]), h), lands, to, lands)

    def land(i):
        for h, origin, to in ((0, down(x), x_up), (1, up(x), x_dn)):
            crossing[i, h]()
            src = relb.at[i, pl.ds(h * 128, 128), :]
            landing.append(send(src, half(group(origin, four[i]), h), to, half(group(far, four[i]), h)))

    unpack(0)
    unpack(1)
    y_other = []
    for wait, rows in ((x_lo, low), (x_hi, high)):
        wait()
        k = other
        y_other.append((
            relay_piece(k, y_up, slot(1 - xl, down(y), c), rows),
            relay_piece(k, y_dn, slot(1 - xl, up(y), c), rows),
        ))
        near.append(relay_piece(k, partner, slot(1 - xl, y, 1 - c), rows))
    z_own[0][0]()
    next_own[0] = onward(0, x)
    z_own[1][1]()
    next_own[1] = onward(1, x)
    forward(0)
    forward(1)
    y_own_dn()
    far_lo = relay_piece(slot(xl, down(y), c), y_up, slot(xl, (y + 2) % 4, c), low)
    near.append(relay_piece(slot(xl, down(y), c), partner, slot(xl, down(y), 1 - c)))
    y_own_up()
    far_hi = relay_piece(slot(xl, up(y), c), y_dn, slot(xl, (y + 2) % 4, c), high)
    near.append(relay_piece(slot(xl, up(y), c), partner, slot(xl, up(y), 1 - c)))
    z_own[2][0]()
    next_own[2] = onward(2, x)
    forward(2)
    z_own[3][1]()
    next_own[3] = onward(3, x)
    cross(0)
    cross(2)
    unpack(2)
    for q in range(3):
        x_far[q]()
        z_far[q] = both(group(far, z), q, far)
        unpack(3 + q)
    z_own[3][0]()
    cross(1)
    land(0)

    def wpart(which, s):
        cols = pl.ds(pl.multiple_of(s * 256, 256), 256)
        near_js = [2 * zz + xh for zz in range(4)]
        far_js = [2 * ((z + i) % 4) + 1 - xh for i in (0, 1, 3)]
        last_js = [2 * ((z + 2) % 4) + 1 - xh]
        js = {"near": near_js, "far": far_js, "last": last_js, "all": near_js + far_js + last_js}[which]
        with jax.named_scope("m" + which):
            at = [pl.ds(pl.multiple_of(j * ROWS, PIECE), ROWS) for j in js]
            if which == "all":
                v = dot(dt[...], cq[:, cols])
            else:
                v = dot(jnp.concatenate([dt[:, a] for a in at], axis=1), jnp.concatenate([cq[a, cols] for a in at], axis=0))
            if which == "near":
                acc[:, cols] = v
            elif which == "far":
                acc[:, cols] += v
            else:
                v = v if which == "all" else v + acc[:, cols]
                zw[:, cols] = (zw[:, cols].astype(F32) * v).astype(BF16)

    for wait in near:
        wait()
    for wait in (z_own[0][1], z_own[1][0], z_own[2][1], next_own[0], next_own[1], next_own[2], next_own[3]):
        wait()
    cross(3)
    land(2)

    @pl.loop(0, 4)
    def _(i):
        wpart("near", jnp.where(i == 3, (1 - xl) * 4 + y, xl * 4 + (y + i + i // 2) % 4))

    passed = []
    k = slot(1 - xl, down(y), c)
    y_other[0][0]()
    far_other_lo = relay_piece(k, y_up, slot(1 - xl, (y + 2) % 4, c), low)
    passed.append(relay_piece(k, partner, slot(1 - xl, down(y), 1 - c), low))
    k = slot(1 - xl, up(y), c)
    y_other[1][1]()
    far_other_hi = relay_piece(k, y_dn, slot(1 - xl, (y + 2) % 4, c), high)
    passed.append(relay_piece(k, partner, slot(1 - xl, up(y), 1 - c), high))
    z_far[0][0]()
    next_far[0] = onward(0, far)
    y_other[1][0]()
    k = slot(1 - xl, down(y), c)
    passed.append(relay_piece(k, partner, slot(1 - xl, down(y), 1 - c), high))
    y_other[0][1]()
    k = slot(1 - xl, up(y), c)
    passed.append(relay_piece(k, partner, slot(1 - xl, up(y), 1 - c), low))
    z_far[1][1]()
    next_far[1] = onward(1, far)
    for wait in passed:
        wait()

    @pl.loop(0, 2)
    def _(i):
        wpart("near", (1 - xl) * 4 + (y + 1 + 2 * i) % 4)

    land(1)
    z_far[2][0]()
    next_far[2] = onward(2, far)
    land(3)
    passed = []
    for wait, rows in ((far_lo, low), (far_hi, high)):
        wait()
        k = slot(xl, (y + 2) % 4, c)
        passed.append(relay_piece(k, partner, slot(xl, (y + 2) % 4, 1 - c), rows))
    for wait in passed:
        wait()

    @pl.loop(0, once)
    def _(_i):
        wpart("near", xl * 4 + (y + 2) % 4)

    for wait in (z_far[0][1], z_far[1][0], z_far[2][1], *landing[:6]):
        wait()
    newest = (1 - xl) * 4 + (y + 2) % 4

    @pl.loop(0, 7)
    def _(i):
        wpart("far", (newest + 1 + i) % 8)

    passed = []
    for wait, rows in ((far_other_lo, low), (far_other_hi, high)):
        wait()
        k = slot(1 - xl, (y + 2) % 4, c)
        passed.append(relay_piece(k, partner, slot(1 - xl, (y + 2) % 4, 1 - c), rows))
    for q in range(3):
        next_far[q]()
    for wait in landing[6:]:
        wait()

    @pl.loop(0, 7)
    def _(i):
        wpart("last", (newest + 1 + i) % 8)

    for wait in passed:
        wait()

    @pl.loop(0, once)
    def _(_i):
        wpart("all", newest)

    for copy in sent:
        copy.wait_send()
    gathered = len(sent)

    def u(t, first, second, col):
        rows = [cq[pl.ds(pl.multiple_of(g * ROWS + t * PIECE, PIECE), PIECE), :] for g in (first, second)]
        with jax.named_scope("u"):
            v = lax.dot_general(
                zw[...], jnp.concatenate(rows, axis=0), (((1,), (1,)), ((), ())), preferred_element_type=F32
            )
            dt[:, pl.ds(pl.multiple_of(col, 256), 256)] = v.astype(BF16)

    def u0(xh):
        @pl.loop(0, 2)
        def _(p):
            u(0, 4 * p + xh, 4 * p + 2 + xh, xh * 512 + p * 256)

    def u2(t, first, count):
        @pl.loop(0, count * once)
        def _(p):
            zz = (first + 2 * p) % 4
            u(t, 2 * zz, 2 * zz + 1, t * 1024 + zz * 256)

    def upart(t, r, h):
        return dt.at[pl.ds(h * 512, 512), pl.ds(pl.multiple_of(t * 1024 + (z + r) % 4 * 256, 256), 256)]

    def uplace(ref, i, h):
        return ref.at[pl.ds(h * 512, 512), i * 256 : (i + 1) * 256]

    moved = {}

    def u_begin(t):
        for h, to in ((0, z_up), (1, z_dn)):
            lands = uplace(uin, t - 1, h)
            moved["in", h, t] = send(upart(t, 2, h), lands, to, lands)

    def u_direct(t):
        for side, r, h, to in ((0, 1, 1, z_up), (1, 3, 0, z_dn)):
            lands = uplace(uf, 2 * side + t - 1, h)
            moved[side, h, t] = send(upart(t, r, h), lands, to, lands)

    def u_pass(t):
        for side, r, h, to in ((0, 1, 0, z_up), (1, 3, 1, z_dn)):
            moved["in", h, t]()
            src = upart(t, r, h)
            src[...] = (src[...].astype(F32) + uplace(uin, t - 1, h)[...].astype(F32)).astype(BF16)
            lands = uplace(uf, 2 * side + t - 1, h)
            moved[side, h, t] = send(src, lands, to, lands)

    def u_end(t):
        for h in range(2):
            moved[0, h, t]()
            moved[1, h, t]()
            src = upart(t, 0, h)
            total = src[...].astype(F32)
            for side in range(2):
                total += uplace(uf, 2 * side + t - 1, h)[...].astype(F32)
            src[...] = total.astype(BF16)

    def lhs(first, second):
        parts = [
            cp[pl.ds(pl.multiple_of(b * ROWS + core * CORE_ROWS, CORE_ROWS), CORE_ROWS), :]
            for core in (1 - c, c) for b in (first, second)
        ]
        return jnp.concatenate(parts, axis=0)

    def store(v, row, col, where, k):
        for p, ref in enumerate((gv, ow)):
            at = pl.ds(pl.multiple_of(where * CORE_ROWS, CORE_ROWS), CORE_ROWS)
            r = p * 384 + row * CORE_ROWS
            ref[at, k * PIECE : (k + 1) * PIECE] = v[r : r + CORE_ROWS, col * PIECE : (col + 1) * PIECE].astype(BF16)

    def k0(r, k):
        to = (x + r) % 4

        @pl.loop(0, 2)
        def _(n):
            with jax.named_scope("k0"):
                first = (to % 2) * 4 + 2 * n
                v = dot(lhs(first, first + 1), dt[:, pl.ds(pl.multiple_of((to // 2) * 512, 512), 512)])
                for b in range(2):
                    for zz in range(4):
                        store(v, b, zz, zz * 4 + 2 * n + b, k)

    def k2(t, k, core, ref):
        @pl.loop(0, 2)
        def _(n):
            with jax.named_scope("k2"):
                rows = [cp[pl.ds(pl.multiple_of((4 * n + b) * ROWS + core * CORE_ROWS, CORE_ROWS), CORE_ROWS), :] for b in range(4)]
                v = dot(jnp.concatenate(rows, axis=0), dt[:, pl.ds(pl.multiple_of(t * 1024 + z * 256, 256), 256)])
                for b in range(4):
                    for hh in range(2):
                        at = pl.ds(pl.multiple_of((b * 4 + hh * 2 + n) * CORE_ROWS, CORE_ROWS), CORE_ROWS)
                        block = v[b * CORE_ROWS : (b + 1) * CORE_ROWS, hh * PIECE : (hh + 1) * PIECE]
                        ref[at, k * PIECE : (k + 1) * PIECE] = block.astype(BF16)

    ups, downs = (x_up, y_up, z_up), (x_dn, y_dn, z_dn)
    place = (x, y, z)
    steps = [(2, 0), (1, 0), (3, 0), (0, 0), (0, 1), (0, 2)]
    index = {s: i for i, s in enumerate(steps)}

    def part(ref, i, start, size):
        return ref.at[pl.ds(start, size), i * PIECE : (i + 1) * PIECE]

    crossed, arrive, held, free = {}, {}, {}, [None] * 4

    def take():
        k = take.next
        take.next = (k + 1) % 4
        if free[k] is not None:
            sent[free[k]].wait_send()
            waited.add(free[k])
        return k

    take.next, waited = 0, set()

    def give(r, t):
        k, i = take(), index[r, t]
        if t:
            k2(t, k, 1 - c, gv)
        else:
            k0(r, k)
        held[i], free[k] = k, len(sent)
        crossed[i] = send(part(gv, k, 0, NBF), part(dr, i, 0, NBF), partner, part(dr, i, 0, NBF))
        if t:
            k2(t, k, c, ow)

    def keep(r, t):
        i = index[r, t]
        crossed[i]()
        k = held[i]

        @pl.loop(0, 4)
        def _(b):
            rows = pl.ds(pl.multiple_of(b * 768, 768), 768)
            at = (rows, slice(i * PIECE, (i + 1) * PIECE))
            dr[at] = (ow[rows, k * PIECE : (k + 1) * PIECE].astype(F32) + dr[at].astype(F32)).astype(BF16)

        if r == 2:
            for h, to in ((0, x_up), (1, x_dn)):
                lands = part(rin1, 0, h * HALF, HALF)
                arrive["in", h] = send(part(dr, i, h * HALF, HALF), lands, to, lands)
        elif r:
            side, h, to = (0, 1, x_up) if r == 1 else (1, 0, x_dn)
            lands = part(rf1, side, h * HALF, HALF)
            arrive[side, h] = send(part(dr, i, h * HALF, HALF), lands, to, lands)

    def pass_on(side):
        r, h, to = ((1, 0, x_up), (3, 1, x_dn))[side]
        i = index[r, 0]
        arrive["in", h]()

        @pl.loop(0, 2)
        def _(b):
            rows = pl.ds(pl.multiple_of(h * HALF + b * 768, 768), 768)
            at = (rows, slice(i * PIECE, (i + 1) * PIECE))
            dr[at] = (dr[at].astype(F32) + rin1[rows, :].astype(F32)).astype(BF16)

        lands = part(rf1, side, h * HALF, HALF)
        arrive[side, h] = send(part(dr, i, h * HALF, HALF), lands, to, lands)

    u2(1, z + 2, 1)
    u_begin(1)
    u0(1 - xh)
    give(2, 0)
    u2(2, z + 2, 1)
    u_begin(2)
    u2(1, z + 1, 2)
    u_direct(1)
    keep(2, 0)
    u0(xh)
    u_pass(1)
    give(1, 0)
    give(3, 0)
    keep(1, 0)
    u2(2, z + 1, 1)
    keep(3, 0)
    u2(2, z + 3, 1)
    u_direct(2)
    pass_on(0)
    pass_on(1)
    u_pass(2)
    u2(1, z, 1)
    u2(2, z, 1)
    give(0, 0)
    u_end(1)
    give(0, 1)
    keep(0, 0)

    second, third = (2, 1, 1), (1, 0, 0)
    base2 = [place[second[t]] * 768 for t in range(3)]
    levels = ((second, 768, rin2, rf2, (0, 0, 0)), (third, 192, None, rf3, base2))
    got = {}

    def summed(level, t, offset, size):
        i = index[0, t]
        row = offset if level == 0 else pl.multiple_of(base2[t] + offset, 32)
        total = dr[pl.ds(row, size), i * PIECE : (i + 1) * PIECE].astype(F32)
        if t == 0:
            for k in range(2):
                total += rf1[pl.ds(row, size), k * PIECE : (k + 1) * PIECE].astype(F32)
        for k in (t, 3 + t):
            if level:
                total += rf2[pl.ds(offset, size), k * PIECE : (k + 1) * PIECE].astype(F32)
        return total

    def put(level, t, offset, v):
        i, base = index[0, t], levels[level][4]
        row = pl.multiple_of(base[t] + offset, 32)
        dr[pl.ds(row, v.shape[0]), i * PIECE : (i + 1) * PIECE] = v.astype(BF16)
        return part(dr, i, row, v.shape[0])

    def begin(level, t, which=(2, 0, 1)):
        axes, size, rin, rf, _ = levels[level]
        half, me = size // 2, place[axes[t]]
        to = ups[axes[t]], downs[axes[t]]
        far = (me + 2) % 4 * size
        for h in range(2) if 2 in which else ():
            at = pl.multiple_of(far + h * half, 32)
            src = put(level, t, at, summed(level, t, at, half))
            lands = part(rin, t, h * half, half)
            got[level, "in", h, t] = send(src, lands, to[h], lands)
        for side, near in ((0, up(me)), (1, down(me))):
            if side not in which:
                continue
            h = 1 - side
            at = pl.multiple_of(near * size + h * half, 32)
            src = put(level, t, at, summed(level, t, at, half))
            lands = part(rf, side * 3 + t, h * half, half)
            got[level, side, h, t] = send(src, lands, to[side], lands)

    def middle(level, t):
        axes, size, rin, rf, _ = levels[level]
        half, me = size // 2, place[axes[t]]
        to = ups[axes[t]], downs[axes[t]]
        for side, near in ((0, up(me)), (1, down(me))):
            h = side
            at = pl.multiple_of(near * size + h * half, 32)
            v = summed(level, t, at, half)
            got[level, "in", h, t]()
            v += rin[h * half : (h + 1) * half, t * PIECE : (t + 1) * PIECE].astype(F32)
            lands = part(rf, side * 3 + t, h * half, half)
            got[level, side, h, t] = send(put(level, t, at, v), lands, to[side], lands)

    def end(level, t):
        for side in range(2):
            for h in range(2):
                got[level, side, h, t]()

    def begin_last(t):
        axis = third[t]
        for n, (d, to) in enumerate(((2, (x_across, y_across)[axis]), (1, ups[axis]), (3, downs[axis]))):
            at = pl.multiple_of((place[axis] + d) % 4 * CORE_ROWS, CORE_ROWS)
            src = put(1, t, at, summed(1, t, at, CORE_ROWS))
            lands = part(rf3, n * 3 + t, 0, CORE_ROWS)
            got["last", n, t] = send(src, lands, to, lands)

    def finish(t):
        total = summed(1, t, pl.multiple_of(place[third[t]] * CORE_ROWS, CORE_ROWS), CORE_ROWS)
        for n in range(3):
            got["last", n, t]()
            total += rf3[:, (n * 3 + t) * PIECE : (n * 3 + t + 1) * PIECE].astype(F32)
        out_ref[:, t * PIECE : (t + 1) * PIECE] = total

    k_last = take()
    i_last = index[0, 2]
    over = {}

    def give_y(dy):
        yy = (y + dy) % 4

        @pl.loop(0, once)
        def _(_i):
            with jax.named_scope("ky"):
                v = dot(lhs(yy, 4 + yy), dt[:, pl.ds(pl.multiple_of(2048 + z * 256, 256), 256)])
                for b in range(2):
                    for hh in range(2):
                        store(v, b, hh, yy * 4 + hh * 2 + b, k_last)

        rows = pl.multiple_of(yy * 768, 768)
        over[dy] = send(part(gv, k_last, rows, 768), part(dr, i_last, rows, 768), partner, part(dr, i_last, rows, 768))

    def keep_y(dy):
        over[dy]()
        rows = pl.ds(pl.multiple_of((y + dy) % 4 * 768, 768), 768)
        at = (rows, slice(i_last * PIECE, (i_last + 1) * PIECE))
        dr[at] = (ow[rows, k_last * PIECE : (k_last + 1) * PIECE].astype(F32) + dr[at].astype(F32)).astype(BF16)

    keep(0, 1)
    begin(0, 1)
    middle(0, 1)
    u_end(2)
    give_y(2)
    give_y(1)
    keep_y(2)
    begin(0, 2, (2,))
    give_y(3)
    keep_y(1)
    begin(0, 2, (0,))
    give_y(0)
    for side in range(2):
        for h in range(2):
            arrive[side, h]()
    begin(0, 0)
    keep_y(3)
    begin(0, 2, (1,))
    keep_y(0)
    middle(0, 2)
    end(0, 1)
    begin_last(1)
    middle(0, 0)
    end(0, 2)
    begin_last(2)
    end(0, 0)
    begin_last(0)
    finish(1)
    finish(2)
    finish(0)

    for i in range(gathered, len(sent)):
        if i not in waited:
            sent[i].wait_send()


def local(collocation, density, kernel_values):
    coefficients = kernel_values.reshape(PANEL * 16, PIECE)
    return pl.pallas_call(
        kernel,
        out_shape=jax.ShapeDtypeStruct((CORE_ROWS, ROWS), F32),
        in_specs=[pl.BlockSpec(memory_space=pl.ANY)] * 3,
        out_specs=pl.BlockSpec(memory_space=pltpu.VMEM),
        scratch_shapes=[
            pltpu.VMEM((NBF, PANEL), BF16),
            pltpu.VMEM((ROWS, NBF), BF16),
            pltpu.VMEM((PANEL, NBF), BF16),
            pltpu.VMEM((NBF, NQ), BF16),
            pltpu.VMEM((PANEL, NQ), BF16),
            pltpu.VMEM((PANEL, NQ), F32),
            pltpu.VMEM((1024, PIECE), F32),
            pltpu.VMEM((3, 256, ROWS), BF16),
            pltpu.VMEM((4, 256, ROWS), BF16),
            pltpu.VMEM((NBF, 4 * PIECE), BF16),
            pltpu.VMEM((NBF, 4 * PIECE), BF16),
            pltpu.VMEM((NBF, 6 * PIECE), BF16),
            pltpu.VMEM((PANEL, 2 * 256), BF16),
            pltpu.VMEM((PANEL, 4 * 256), BF16),
            pltpu.VMEM((NBF, PIECE), BF16),
            pltpu.VMEM((NBF, 2 * PIECE), BF16),
            pltpu.VMEM((768, 3 * PIECE), BF16),
            pltpu.VMEM((768, 6 * PIECE), BF16),
            pltpu.VMEM((192, 9 * PIECE), BF16),
            pltpu.SemaphoreType.DMA((N_SENDS,)),
            pltpu.SemaphoreType.DMA((N_SENDS,)),
            pltpu.SemaphoreType.DMA((12,)),
        ],
        compiler_params=pltpu.CompilerParams(
            collective_id=0, has_side_effects=True, vmem_limit_bytes=67043328
        ),
    )(collocation, density, coefficients)


def solution(mesh):
    return jax.shard_map(
        local,
        mesh=mesh,
        in_specs=(P(None, "gx"), P("gy", None), P("gx", None, "gy", None)),
        out_specs=P("gx", "gy"),
        check_vma=False,
    )
```

```python
import jax
import jax.numpy as jnp
from jax import lax
from jax.experimental import pallas as pl
from jax.experimental.pallas import tpu as pltpu
from jax.sharding import PartitionSpec as P

MESH = pl.DeviceIdType.MESH
BF16 = jnp.bfloat16
F32 = jnp.float32

NBF = 3072
PANEL = 1024
PIECE = 128
ROWS = 384
NQ = 2048
HALF = NBF // 2
CORE_ROWS = 192
N_SENDS = 160


def dot(a, b):
    return jnp.dot(a, b, preferred_element_type=F32)


def kernel(
    c_ref, d_ref, z_ref, out_ref,
    cp, dv, dt, cq, zw, acc, zf, rel, relb, gv, ow, dr, uin, uf, rin1, rf1, rin2, rf2, rf3,
    send_sem, recv_sem, local_sem,
):
    gx, gy = lax.axis_index("gx"), lax.axis_index("gy")
    c, y, xl = gx % 2, (gx // 2) % 4, gx // 8
    z, xh = gy // 2, gy % 2
    x = xh * 2 + xl
    once = 1 + gx // 16

    def device(x, y, z, c):
        return {"gx": ((x % 2) * 4 + y) * 2 + c, "gy": z * 2 + x // 2}

    def up(v):
        return (v + 1) % 4

    def down(v):
        return (v + 3) % 4

    partner = device(x, y, z, 1 - c)
    x_up, x_dn = device(up(x), y, z, c), device(down(x), y, z, c)
    y_up, y_dn = device(x, up(y), z, c), device(x, down(y), z, c)
    z_up, z_dn = device(x, y, up(z), c), device(x, y, down(z), c)

    x_across, y_across = device((x + 2) % 4, y, z, c), device(x, (y + 2) % 4, z, c)

    barrier = pltpu.get_barrier_semaphore()
    neighbours = (x_across, y_across, partner, x_up, x_dn, y_up, y_dn, z_up, z_dn)
    for one in neighbours:
        pl.semaphore_signal(barrier, inc=1, device_id=one, device_id_type=MESH)

    locals_ = []

    def fetch(src, dst):
        copy = pltpu.make_async_copy(src, dst, local_sem.at[len(locals_)])
        copy.start()
        locals_.append(copy)
        return copy

    def column(ref, k, rows=None, width=PIECE):
        cols = pl.ds(pl.multiple_of(k * width, PIECE), width)
        return ref.at[:, cols] if rows is None else ref.at[pl.ds(*rows), cols]

    d_in = fetch(d_ref, dv)
    cp_in = [fetch(column(c_ref, i, width=256), column(cp, i, width=256)) for i in range(4)]
    own_in = fetch(column(c_ref, gy), column(cq, gx))
    sent = []

    def send(src, dst, to, lands):
        i = len(sent)
        copy = pltpu.make_async_remote_copy(
            src_ref=src, dst_ref=dst, send_sem=send_sem.at[i], recv_sem=recv_sem.at[i],
            device_id=to, device_id_type=MESH,
        )
        copy.start()
        sent.append(copy)
        arrival = pltpu.make_async_remote_copy(
            src_ref=lands, dst_ref=lands, send_sem=send_sem.at[i], recv_sem=recv_sem.at[i],
            device_id=to, device_id_type=MESH,
        )
        return arrival.wait_recv

    def slot(xl, y, c):
        return (xl * 4 + y) * 2 + c

    low, high = (0, HALF), (HALF, HALF)

    def piece(k, rows=None):
        return column(cq, k, rows)

    def relay_piece(k, to, mine, rows=None):
        return send(piece(k, rows), piece(k, rows), to, piece(mine, rows))

    own_cols = pl.ds(pl.multiple_of(gy * ROWS, PIECE), ROWS)

    def dense(q):
        cp_in[q].wait()

        @pl.loop(0, once)
        def _(_i):
            with jax.named_scope(f"own{q}"):
                rows = dot(dv[...], cp[:, q * 256 : (q + 1) * 256])
                dt[q * 256 : (q + 1) * 256, own_cols] = rows.T.astype(BF16)

    d_in.wait()
    dense(0)
    pl.semaphore_wait(barrier, len(neighbours))

    own_in.wait()
    own = piece(gx)
    y_own_dn = send(own, piece(gx), y_up, piece(slot(xl, down(y), c)))
    y_own_up = send(own, piece(gx), y_dn, piece(slot(xl, up(y), c)))
    other = slot(1 - xl, y, c)
    x_lo = send(column(c_ref, z * 2 + up(x) // 2, low), piece(gx, low), x_up, piece(other, low))
    x_hi = send(column(c_ref, z * 2 + down(x) // 2, high), piece(gx, high), x_dn, piece(other, high))
    near = [send(own, piece(gx), partner, piece(slot(xl, y, 1 - c)))]

    def block(j, q):
        return dt.at[pl.ds(q * 256, 256), pl.ds(pl.multiple_of(j * ROWS, PIECE), ROWS)]

    def group(x, z):
        return z * 2 + x // 2

    def both(j, q, xz):
        return (
            send(block(j, q), block(j, q), z_up, block(group(xz, down(z)), q)),
            send(block(j, q), block(j, q), z_dn, block(group(xz, up(z)), q)),
        )

    def onward(q, xz):
        b = block(group(xz, (down(z), up(z))[q % 2]), q)
        return send(b, b, (z_up, z_dn)[q % 2], block(group(xz, (z + 2) % 4), q))

    z_own, relayed = [], []
    for q in range(4):
        if q:
            dense(q)
        z_own.append(both(gy, q, x))
        if q < 3:
            relayed.append(send(block(gy, q), rel.at[q], (x_up, x_dn)[q % 2], rel.at[q]))

    z_in = []
    for i in range(6):
        ref, rows = (gv, ow)[i // 4], min(NBF, PANEL * 16 - i * NBF)
        z_in.append(fetch(z_ref.at[pl.ds(i * NBF, rows)], column(ref, i % 4, (0, rows))))

    def unpack(i):
        ref, n = (gv, ow)[i // 4], min(CORE_ROWS, PANEL - i * CORE_ROWS)
        z_in[i].wait()

        @pl.loop(0, n // 64)
        def _(b):
            with jax.named_scope("unpack"):
                first = pl.multiple_of(b * 1024, 1024)
                zf[...] = ref[pl.ds(first, 1024), (i % 4) * PIECE : (i % 4 + 1) * PIECE].astype(F32)
                to = pl.ds(pl.multiple_of(i * CORE_ROWS + b * 64, 64), 64)
                for k in range(16):
                    zw[to, k * PIECE : (k + 1) * PIECE] = zf[pl.ds(k, 64, stride=16), :].astype(BF16)

    x_far, z_far, next_own, next_far = {}, {}, {}, {}
    far = (x + 2) % 4

    def forward(q):
        relayed[q]()
        origin = group((down(x), up(x))[q % 2], z)
        x_far[q] = send(rel.at[q], block(origin, q), (x_up, x_dn)[q % 2], block(group(far, z), q))

    four = (z, down(z), up(z), (z + 2) % 4)
    crossing, landing = {}, []

    def half(j, h):
        return dt.at[pl.ds(768 + h * 128, 128), pl.ds(pl.multiple_of(j * ROWS, PIECE), ROWS)]

    def cross(i):
        for h, to in ((0, x_up), (1, x_dn)):
            lands = relb.at[i, pl.ds(h * 128, 128), :]
            crossing[i, h] = send(half(group(x, four[i]), h), lands, to, lands)

    def land(i):
        for h, origin, to in ((0, down(x), x_up), (1, up(x), x_dn)):
            crossing[i, h]()
            src = relb.at[i, pl.ds(h * 128, 128), :]
            landing.append(send(src, half(group(origin, four[i]), h), to, half(group(far, four[i]), h)))

    unpack(0)
    unpack(1)
    y_other = []
    for wait, rows in ((x_lo, low), (x_hi, high)):
        wait()
        k = other
        y_other.append((
            relay_piece(k, y_up, slot(1 - xl, down(y), c), rows),
            relay_piece(k, y_dn, slot(1 - xl, up(y), c), rows),
        ))
        near.append(relay_piece(k, partner, slot(1 - xl, y, 1 - c), rows))
    z_own[0][0]()
    next_own[0] = onward(0, x)
    z_own[1][1]()
    next_own[1] = onward(1, x)
    forward(0)
    forward(1)
    y_own_dn()
    far_lo = relay_piece(slot(xl, down(y), c), y_up, slot(xl, (y + 2) % 4, c), low)
    near.append(relay_piece(slot(xl, down(y), c), partner, slot(xl, down(y), 1 - c)))
    y_own_up()
    far_hi = relay_piece(slot(xl, up(y), c), y_dn, slot(xl, (y + 2) % 4, c), high)
    near.append(relay_piece(slot(xl, up(y), c), partner, slot(xl, up(y), 1 - c)))
    z_own[2][0]()
    next_own[2] = onward(2, x)
    forward(2)
    z_own[3][1]()
    next_own[3] = onward(3, x)
    cross(0)
    cross(2)
    unpack(2)
    for q in range(3):
        x_far[q]()
        z_far[q] = both(group(far, z), q, far)
        unpack(3 + q)
    z_own[3][0]()
    cross(1)
    land(0)

    def wpart(which, s):
        cols = pl.ds(pl.multiple_of(s * 256, 256), 256)
        near_js = [2 * zz + xh for zz in range(4)]
        far_js = [2 * ((z + i) % 4) + 1 - xh for i in (0, 1, 3)]
        last_js = [2 * ((z + 2) % 4) + 1 - xh]
        js = {"near": near_js, "far": far_js, "last": last_js, "all": near_js + far_js + last_js}[which]
        with jax.named_scope("m" + which):
            at = [pl.ds(pl.multiple_of(j * ROWS, PIECE), ROWS) for j in js]
            if which == "all":
                v = dot(dt[...], cq[:, cols])
            else:
                v = dot(jnp.concatenate([dt[:, a] for a in at], axis=1), jnp.concatenate([cq[a, cols] for a in at], axis=0))
            if which == "near":
                acc[:, cols] = v
            elif which == "far":
                acc[:, cols] += v
            else:
                v = v if which == "all" else v + acc[:, cols]
                zw[:, cols] = (zw[:, cols].astype(F32) * v).astype(BF16)

    for wait in near:
        wait()
    for wait in (z_own[0][1], z_own[1][0], z_own[2][1], next_own[0], next_own[1], next_own[2], next_own[3]):
        wait()
    cross(3)
    land(2)

    @pl.loop(0, 4)
    def _(i):
        wpart("near", jnp.where(i == 3, (1 - xl) * 4 + y, xl * 4 + (y + i + i // 2) % 4))

    passed = []
    k = slot(1 - xl, down(y), c)
    y_other[0][0]()
    far_other_lo = relay_piece(k, y_up, slot(1 - xl, (y + 2) % 4, c), low)
    passed.append(relay_piece(k, partner, slot(1 - xl, down(y), 1 - c), low))
    k = slot(1 - xl, up(y), c)
    y_other[1][1]()
    far_other_hi = relay_piece(k, y_dn, slot(1 - xl, (y + 2) % 4, c), high)
    passed.append(relay_piece(k, partner, slot(1 - xl, up(y), 1 - c), high))
    z_far[0][0]()
    next_far[0] = onward(0, far)
    y_other[1][0]()
    k = slot(1 - xl, down(y), c)
    passed.append(relay_piece(k, partner, slot(1 - xl, down(y), 1 - c), high))
    y_other[0][1]()
    k = slot(1 - xl, up(y), c)
    passed.append(relay_piece(k, partner, slot(1 - xl, up(y), 1 - c), low))
    z_far[1][1]()
    next_far[1] = onward(1, far)
    for wait in passed:
        wait()

    @pl.loop(0, 2)
    def _(i):
        wpart("near", (1 - xl) * 4 + (y + 1 + 2 * i) % 4)

    land(1)
    z_far[2][0]()
    next_far[2] = onward(2, far)
    land(3)
    passed = []
    for wait, rows in ((far_lo, low), (far_hi, high)):
        wait()
        k = slot(xl, (y + 2) % 4, c)
        passed.append(relay_piece(k, partner, slot(xl, (y + 2) % 4, 1 - c), rows))
    for wait in passed:
        wait()

    @pl.loop(0, once)
    def _(_i):
        wpart("near", xl * 4 + (y + 2) % 4)

    for wait in (z_far[0][1], z_far[1][0], z_far[2][1], *landing[:6]):
        wait()
    newest = (1 - xl) * 4 + (y + 2) % 4

    @pl.loop(0, 7)
    def _(i):
        wpart("far", (newest + 1 + i) % 8)

    passed = []
    for wait, rows in ((far_other_lo, low), (far_other_hi, high)):
        wait()
        k = slot(1 - xl, (y + 2) % 4, c)
        passed.append(relay_piece(k, partner, slot(1 - xl, (y + 2) % 4, 1 - c), rows))
    for q in range(3):
        next_far[q]()
    for wait in landing[6:]:
        wait()

    @pl.loop(0, 7)
    def _(i):
        wpart("last", (newest + 1 + i) % 8)

    for wait in passed:
        wait()

    @pl.loop(0, once)
    def _(_i):
        wpart("all", newest)

    for copy in sent:
        copy.wait_send()
    gathered = len(sent)

    def u(t, first, second, col):
        rows = [cq[pl.ds(pl.multiple_of(g * ROWS + t * PIECE, PIECE), PIECE), :] for g in (first, second)]
        with jax.named_scope("u"):
            v = lax.dot_general(
                zw[...], jnp.concatenate(rows, axis=0), (((1,), (1,)), ((), ())), preferred_element_type=F32
            )
            dt[:, pl.ds(pl.multiple_of(col, 256), 256)] = v.astype(BF16)

    def u0(xh):
        @pl.loop(0, 2)
        def _(p):
            u(0, 4 * p + xh, 4 * p + 2 + xh, xh * 512 + p * 256)

    def u2(t, first, count):
        @pl.loop(0, count * once)
        def _(p):
            zz = (first + 2 * p) % 4
            u(t, 2 * zz, 2 * zz + 1, t * 1024 + zz * 256)

    def upart(t, r, h):
        return dt.at[pl.ds(h * 512, 512), pl.ds(pl.multiple_of(t * 1024 + (z + r) % 4 * 256, 256), 256)]

    def uplace(ref, i, h):
        return ref.at[pl.ds(h * 512, 512), i * 256 : (i + 1) * 256]

    moved = {}

    def u_begin(t):
        for h, to in ((0, z_up), (1, z_dn)):
            lands = uplace(uin, t - 1, h)
            moved["in", h, t] = send(upart(t, 2, h), lands, to, lands)

    def u_direct(t):
        for side, r, h, to in ((0, 1, 1, z_up), (1, 3, 0, z_dn)):
            lands = uplace(uf, 2 * side + t - 1, h)
            moved[side, h, t] = send(upart(t, r, h), lands, to, lands)

    def u_pass(t):
        for side, r, h, to in ((0, 1, 0, z_up), (1, 3, 1, z_dn)):
            moved["in", h, t]()
            src = upart(t, r, h)
            src[...] = (src[...].astype(F32) + uplace(uin, t - 1, h)[...].astype(F32)).astype(BF16)
            lands = uplace(uf, 2 * side + t - 1, h)
            moved[side, h, t] = send(src, lands, to, lands)

    def u_end(t):
        for h in range(2):
            moved[0, h, t]()
            moved[1, h, t]()
            src = upart(t, 0, h)
            total = src[...].astype(F32)
            for side in range(2):
                total += uplace(uf, 2 * side + t - 1, h)[...].astype(F32)
            src[...] = total.astype(BF16)

    def lhs(first, second):
        parts = [
            cp[pl.ds(pl.multiple_of(b * ROWS + core * CORE_ROWS, CORE_ROWS), CORE_ROWS), :]
            for core in (1 - c, c) for b in (first, second)
        ]
        return jnp.concatenate(parts, axis=0)

    def store(v, row, col, where, k):
        for p, ref in enumerate((gv, ow)):
            at = pl.ds(pl.multiple_of(where * CORE_ROWS, CORE_ROWS), CORE_ROWS)
            r = p * 384 + row * CORE_ROWS
            ref[at, k * PIECE : (k + 1) * PIECE] = v[r : r + CORE_ROWS, col * PIECE : (col + 1) * PIECE].astype(BF16)

    def k0(r, k):
        to = (x + r) % 4

        @pl.loop(0, 2)
        def _(n):
            with jax.named_scope("k0"):
                first = (to % 2) * 4 + 2 * n
                v = dot(lhs(first, first + 1), dt[:, pl.ds(pl.multiple_of((to // 2) * 512, 512), 512)])
                for b in range(2):
                    for zz in range(4):
                        store(v, b, zz, zz * 4 + 2 * n + b, k)

    def k2(t, k, core, ref):
        @pl.loop(0, 2)
        def _(n):
            with jax.named_scope("k2"):
                rows = [cp[pl.ds(pl.multiple_of((4 * n + b) * ROWS + core * CORE_ROWS, CORE_ROWS), CORE_ROWS), :] for b in range(4)]
                v = dot(jnp.concatenate(rows, axis=0), dt[:, pl.ds(pl.multiple_of(t * 1024 + z * 256, 256), 256)])
                for b in range(4):
                    for hh in range(2):
                        at = pl.ds(pl.multiple_of((b * 4 + hh * 2 + n) * CORE_ROWS, CORE_ROWS), CORE_ROWS)
                        block = v[b * CORE_ROWS : (b + 1) * CORE_ROWS, hh * PIECE : (hh + 1) * PIECE]
                        ref[at, k * PIECE : (k + 1) * PIECE] = block.astype(BF16)

    ups, downs = (x_up, y_up, z_up), (x_dn, y_dn, z_dn)
    place = (x, y, z)
    steps = [(2, 0), (1, 0), (3, 0), (0, 0), (0, 1), (0, 2)]
    index = {s: i for i, s in enumerate(steps)}

    def part(ref, i, start, size):
        return ref.at[pl.ds(start, size), i * PIECE : (i + 1) * PIECE]

    crossed, arrive, held, free = {}, {}, {}, [None] * 4

    def take():
        k = take.next
        take.next = (k + 1) % 4
        if free[k] is not None:
            sent[free[k]].wait_send()
            waited.add(free[k])
        return k

    take.next, waited = 0, set()

    def give(r, t):
        k, i = take(), index[r, t]
        if t:
            k2(t, k, 1 - c, gv)
        else:
            k0(r, k)
        held[i], free[k] = k, len(sent)
        crossed[i] = send(part(gv, k, 0, NBF), part(dr, i, 0, NBF), partner, part(dr, i, 0, NBF))
        if t:
            k2(t, k, c, ow)

    def keep(r, t):
        i = index[r, t]
        crossed[i]()
        k = held[i]

        @pl.loop(0, 4)
        def _(b):
            rows = pl.ds(pl.multiple_of(b * 768, 768), 768)
            at = (rows, slice(i * PIECE, (i + 1) * PIECE))
            dr[at] = (ow[rows, k * PIECE : (k + 1) * PIECE].astype(F32) + dr[at].astype(F32)).astype(BF16)

        if r == 2:
            for h, to in ((0, x_up), (1, x_dn)):
                lands = part(rin1, 0, h * HALF, HALF)
                arrive["in", h] = send(part(dr, i, h * HALF, HALF), lands, to, lands)
        elif r:
            side, h, to = (0, 1, x_up) if r == 1 else (1, 0, x_dn)
            lands = part(rf1, side, h * HALF, HALF)
            arrive[side, h] = send(part(dr, i, h * HALF, HALF), lands, to, lands)

    def pass_on(side):
        r, h, to = ((1, 0, x_up), (3, 1, x_dn))[side]
        i = index[r, 0]
        arrive["in", h]()

        @pl.loop(0, 2)
        def _(b):
            rows = pl.ds(pl.multiple_of(h * HALF + b * 768, 768), 768)
            at = (rows, slice(i * PIECE, (i + 1) * PIECE))
            dr[at] = (dr[at].astype(F32) + rin1[rows, :].astype(F32)).astype(BF16)

        lands = part(rf1, side, h * HALF, HALF)
        arrive[side, h] = send(part(dr, i, h * HALF, HALF), lands, to, lands)

    u2(1, z + 2, 1)
    u_begin(1)
    u0(1 - xh)
    give(2, 0)
    u2(2, z + 2, 1)
    u_begin(2)
    u2(1, z + 1, 1)
    keep(2, 0)
    u2(1, z + 3, 1)
    u_direct(1)
    u0(xh)
    u_pass(1)
    give(1, 0)
    give(3, 0)
    keep(1, 0)
    u2(2, z + 1, 1)
    keep(3, 0)
    u2(2, z + 3, 1)
    u_direct(2)
    pass_on(0)
    pass_on(1)
    u_pass(2)
    u2(1, z, 1)
    u2(2, z, 1)
    give(0, 0)
    u_end(1)
    give(0, 1)
    keep(0, 0)

    second, third = (2, 1, 1), (1, 0, 0)
    base2 = [place[second[t]] * 768 for t in range(3)]
    levels = ((second, 768, rin2, rf2, (0, 0, 0)), (third, 192, None, rf3, base2))
    got = {}

    def summed(level, t, offset, size):
        i = index[0, t]
        row = offset if level == 0 else pl.multiple_of(base2[t] + offset, 32)
        total = dr[pl.ds(row, size), i * PIECE : (i + 1) * PIECE].astype(F32)
        if t == 0:
            for k in range(2):
                total += rf1[pl.ds(row, size), k * PIECE : (k + 1) * PIECE].astype(F32)
        for k in (t, 3 + t):
            if level:
                total += rf2[pl.ds(offset, size), k * PIECE : (k + 1) * PIECE].astype(F32)
        return total

    def put(level, t, offset, v):
        i, base = index[0, t], levels[level][4]
        row = pl.multiple_of(base[t] + offset, 32)
        dr[pl.ds(row, v.shape[0]), i * PIECE : (i + 1) * PIECE] = v.astype(BF16)
        return part(dr, i, row, v.shape[0])

    def begin(level, t, which=(2, 0, 1)):
        axes, size, rin, rf, _ = levels[level]
        half, me = size // 2, place[axes[t]]
        to = ups[axes[t]], downs[axes[t]]
        far = (me + 2) % 4 * size
        for h in range(2) if 2 in which else ():
            at = pl.multiple_of(far + h * half, 32)
            src = put(level, t, at, summed(level, t, at, half))
            lands = part(rin, t, h * half, half)
            got[level, "in", h, t] = send(src, lands, to[h], lands)
        for side, near in ((0, up(me)), (1, down(me))):
            if side not in which:
                continue
            h = 1 - side
            at = pl.multiple_of(near * size + h * half, 32)
            src = put(level, t, at, summed(level, t, at, half))
            lands = part(rf, side * 3 + t, h * half, half)
            got[level, side, h, t] = send(src, lands, to[side], lands)

    def middle(level, t):
        axes, size, rin, rf, _ = levels[level]
        half, me = size // 2, place[axes[t]]
        to = ups[axes[t]], downs[axes[t]]
        for side, near in ((0, up(me)), (1, down(me))):
            h = side
            at = pl.multiple_of(near * size + h * half, 32)
            v = summed(level, t, at, half)
            got[level, "in", h, t]()
            v += rin[h * half : (h + 1) * half, t * PIECE : (t + 1) * PIECE].astype(F32)
            lands = part(rf, side * 3 + t, h * half, half)
            got[level, side, h, t] = send(put(level, t, at, v), lands, to[side], lands)

    def end(level, t):
        for side in range(2):
            for h in range(2):
                got[level, side, h, t]()

    def begin_last(t):
        axis = third[t]
        for n, (d, to) in enumerate(((2, (x_across, y_across)[axis]), (1, ups[axis]), (3, downs[axis]))):
            at = pl.multiple_of((place[axis] + d) % 4 * CORE_ROWS, CORE_ROWS)
            src = put(1, t, at, summed(1, t, at, CORE_ROWS))
            lands = part(rf3, n * 3 + t, 0, CORE_ROWS)
            got["last", n, t] = send(src, lands, to, lands)

    def finish(t):
        total = summed(1, t, pl.multiple_of(place[third[t]] * CORE_ROWS, CORE_ROWS), CORE_ROWS)
        for n in range(3):
            got["last", n, t]()
            total += rf3[:, (n * 3 + t) * PIECE : (n * 3 + t + 1) * PIECE].astype(F32)
        out_ref[:, t * PIECE : (t + 1) * PIECE] = total

    k_last = take()
    i_last = index[0, 2]
    over = {}

    def give_y(dy):
        yy = (y + dy) % 4

        @pl.loop(0, once)
        def _(_i):
            with jax.named_scope("ky"):
                v = dot(lhs(yy, 4 + yy), dt[:, pl.ds(pl.multiple_of(2048 + z * 256, 256), 256)])
                for b in range(2):
                    for hh in range(2):
                        store(v, b, hh, yy * 4 + hh * 2 + b, k_last)

        rows = pl.multiple_of(yy * 768, 768)
        over[dy] = send(part(gv, k_last, rows, 768), part(dr, i_last, rows, 768), partner, part(dr, i_last, rows, 768))

    def keep_y(dy):
        over[dy]()
        rows = pl.ds(pl.multiple_of((y + dy) % 4 * 768, 768), 768)
        at = (rows, slice(i_last * PIECE, (i_last + 1) * PIECE))
        dr[at] = (ow[rows, k_last * PIECE : (k_last + 1) * PIECE].astype(F32) + dr[at].astype(F32)).astype(BF16)

    keep(0, 1)
    begin(0, 1)
    middle(0, 1)
    u_end(2)
    give_y(2)
    give_y(1)
    keep_y(2)
    begin(0, 2, (2,))
    give_y(3)
    keep_y(1)
    begin(0, 2, (0,))
    give_y(0)
    for side in range(2):
        for h in range(2):
            arrive[side, h]()
    begin(0, 0)
    keep_y(3)
    begin(0, 2, (1,))
    keep_y(0)
    middle(0, 2)
    end(0, 1)
    begin_last(1)
    middle(0, 0)
    end(0, 2)
    begin_last(2)
    end(0, 0)
    begin_last(0)
    finish(1)
    finish(2)
    finish(0)

    for i in range(gathered, len(sent)):
        if i not in waited:
            sent[i].wait_send()


def local(collocation, density, kernel_values):
    coefficients = kernel_values.reshape(PANEL * 16, PIECE)
    return pl.pallas_call(
        kernel,
        out_shape=jax.ShapeDtypeStruct((CORE_ROWS, ROWS), F32),
        in_specs=[pl.BlockSpec(memory_space=pl.ANY)] * 3,
        out_specs=pl.BlockSpec(memory_space=pltpu.VMEM),
        scratch_shapes=[
            pltpu.VMEM((NBF, PANEL), BF16),
            pltpu.VMEM((ROWS, NBF), BF16),
            pltpu.VMEM((PANEL, NBF), BF16),
            pltpu.VMEM((NBF, NQ), BF16),
            pltpu.VMEM((PANEL, NQ), BF16),
            pltpu.VMEM((PANEL, NQ), F32),
            pltpu.VMEM((1024, PIECE), F32),
            pltpu.VMEM((3, 256, ROWS), BF16),
            pltpu.VMEM((4, 256, ROWS), BF16),
            pltpu.VMEM((NBF, 4 * PIECE), BF16),
            pltpu.VMEM((NBF, 4 * PIECE), BF16),
            pltpu.VMEM((NBF, 6 * PIECE), BF16),
            pltpu.VMEM((PANEL, 2 * 256), BF16),
            pltpu.VMEM((PANEL, 4 * 256), BF16),
            pltpu.VMEM((NBF, PIECE), BF16),
            pltpu.VMEM((NBF, 2 * PIECE), BF16),
            pltpu.VMEM((768, 3 * PIECE), BF16),
            pltpu.VMEM((768, 6 * PIECE), BF16),
            pltpu.VMEM((192, 9 * PIECE), BF16),
            pltpu.SemaphoreType.DMA((N_SENDS,)),
            pltpu.SemaphoreType.DMA((N_SENDS,)),
            pltpu.SemaphoreType.DMA((12,)),
        ],
        compiler_params=pltpu.CompilerParams(
            collective_id=0, has_side_effects=True, vmem_limit_bytes=67043328
        ),
    )(collocation, density, coefficients)


def solution(mesh):
    return jax.shard_map(
        local,
        mesh=mesh,
        in_specs=(P(None, "gx"), P("gy", None), P("gx", None, "gy", None)),
        out_specs=P("gx", "gy"),
        check_vma=False,
    )
```
